256 devices in a mesh: dp: 32 (over x, y, core), table: 8 (over z).
Axes of the slice: x: 4, y: 4, z: 8, core: 2. Of those that a mesh axis runs over, the one named last changes fastest.
Arguments:
- item_ids: int32 [512, 384], P(('dp', 'table')), may hold values from 0 to 3145727, as said below
- table_ids: int32 [512, 384], P(('dp', 'table')), may hold values from 0 to 3
- lengths: int32 [512], P(('dp', 'table')), may hold values from 24 to 384
- assignment: int32 [512], P(('dp', 'table')), may hold values from 0 to 511, as said below
- table_a: bfloat16 [3145728, 64], P(('dp', 'table')), may hold values from -6 to 6
- table_b: bfloat16 [3145728, 64], P(('dp', 'table')), may hold values from -6 to 6
- table_c: bfloat16 [1572864, 128], P(('dp', 'table')), may hold values from -6 to 6
- table_d: bfloat16 [524288, 256], P(('dp', 'table')), may hold values from -6 to 6
- proj_weight: bfloat16 [512, 512], P('dp'), may hold values from -0.5 to 0.5
- in_weight: bfloat16 [512, 2048], P('dp'), may hold values from -0.25 to 0.25
- out_weight: bfloat16 [512, 512], P('dp'), may hold values from -0.25 to 0.25
- cotangent: bfloat16 [512, 384, 512], P(('dp', 'table')), may hold values from -24 to 24
Outputs:
- output: bfloat16 [512, 384, 512], P(('dp', 'table'))
- grad_a: bfloat16 [3145728, 64], P(('dp', 'table'))
- grad_b: bfloat16 [3145728, 64], P(('dp', 'table'))
- grad_c: bfloat16 [1572864, 128], P(('dp', 'table'))
- grad_d: bfloat16 [524288, 256], P(('dp', 'table'))
- grad_proj: float32 [512, 512], P('dp')
- grad_in: float32 [512, 2048], P('dp')
- grad_out: float32 [512, 512], P('dp')
The draws below stay inside these ranges and needn't reach their ends.
Inputs may be any that keep to these rules, and one draw needn't show every extreme that they name: `item_ids`: A sequence's events past its length name rows too. An event's item is below 256 times the rows one device holds of the event's table (row r of a table lies on device r // (rows a device of that table) along dp+table). After the move, the events of the 2 slots of one device name at most 2 times rows of one table held by one device, and for some table and device exactly 2 times, from every device. `assignment`: A permutation of the sequence slots; a sequence moves only among the devices of its own table index, and each device receives 2 sequences.
All inputs are finite; a program needn't handle non-finite values.
Results may differ from the reference program's by a relative error of at most 0.028.
Values may be sent and summed in bfloat16 or wider, within the bound.
A program may use at most 128 MiB of HBM per device.

```python
import jax
import jax.numpy as jnp
from jax import lax

D = 512
HEADS = 4
FF = 2048
WIDTH_A = 64
WIDTH_B = 64
WIDTH_C = 128
WIDTH_D = 256
WSUM = 512
ROWS_A = 12288
ROWS_B = 12288
ROWS_C = 6144
ROWS_D = 2048
MAXLEN = 384
SEQ_DEV = 2
SEQS = 512
CAP = 2
TROWS_A = 3145728
TROWS_B = 3145728
TROWS_C = 1572864
TROWS_D = 524288
N_DP = 32
N_TABLE = 8
DEVICES = 256


def build_layout(key):
    base = jax.random.fold_in(key, 4242)
    subkeys = jax.random.split(base, 5)
    seq_total = SEQ_DEV * DEVICES
    tok_total = SEQ_DEV * MAXLEN
    seq_index = jnp.arange(seq_total, dtype=jnp.int32)
    seq_lengths = jax.random.randint(subkeys[0], (seq_total,), MAXLEN // 16, MAXLEN + 1, dtype=jnp.int32)
    group_of = seq_index // SEQ_DEV % N_TABLE
    sort_key = group_of * ((MAXLEN + 2) * seq_total) + (MAXLEN + 1 - seq_lengths) * seq_total + seq_index
    ordering = jnp.argsort(sort_key)
    seq_rank = jnp.zeros((seq_total,), jnp.int32).at[ordering].set(seq_index)
    in_group = seq_rank - group_of * (N_DP * SEQ_DEV)
    rounds = in_group // N_DP
    position = in_group % N_DP
    device_of = jnp.where(rounds % 2 == 0, position, N_DP - 1 - position)
    targets = (device_of * N_TABLE + group_of) * SEQ_DEV + rounds
    slot_total = 4 * DEVICES * CAP
    bucket = jnp.arange(slot_total, dtype=jnp.int32) // CAP
    special = jax.random.randint(subkeys[1], (), 0, 4 * DEVICES, dtype=jnp.int32)
    noise_bits = jax.random.randint(subkeys[2], (DEVICES, slot_total), 0, (1 << 30) // slot_total, dtype=jnp.int32)
    scores = jnp.where(bucket[None, :] == special, -slot_total, noise_bits * slot_total) + jnp.arange(slot_total, dtype=jnp.int32)[None, :]
    picked = jnp.argsort(scores, axis=1)[:, :tok_total]
    chosen = bucket[picked]
    shuffle_bits = jax.random.randint(subkeys[3], (DEVICES, tok_total), 0, (1 << 30) // tok_total, dtype=jnp.int32)
    shuffle = jnp.argsort(shuffle_bits * tok_total + jnp.arange(tok_total, dtype=jnp.int32)[None, :], axis=1)
    chosen = jnp.take_along_axis(chosen, shuffle, axis=1)
    table_of = chosen % 4
    owners = chosen // 4
    row_limit = jnp.where(table_of == 0, ROWS_A, jnp.where(table_of == 1, ROWS_B, jnp.where(table_of == 2, ROWS_C, ROWS_D)))
    local_row = jax.random.randint(subkeys[4], (DEVICES, tok_total), 0, 1 << 30, dtype=jnp.int32) % row_limit
    item_rows = (owners * row_limit + local_row).reshape(seq_total, MAXLEN)[targets]
    table_rows = table_of.reshape(seq_total, MAXLEN)[targets]
    return (seq_lengths, targets, item_rows, table_rows)


def draw_lengths(key, part):
    return build_layout(key)[0]


def draw_assignment(key, part):
    return build_layout(key)[1]


def draw_item_ids(key, part):
    return build_layout(key)[2]


def draw_table_ids(key, part):
    return build_layout(key)[3]


def strengthened(values, key, source, target, shards_of, factor):
    def block_of(axis_at):
        return (jnp.arange(values.shape[axis_at]) // (values.shape[axis_at] // shards_of)).reshape((-1,) + (1,) * (values.ndim - 1 - axis_at))

    one_side = jax.random.permutation(key, shards_of)[block_of(target)]
    second = (block_of(target) + shards_of // 2) % shards_of
    return jnp.where((block_of(source) == one_side) | (block_of(source) == second), factor * values, values)


def steps_of(own_key, dims, shards, smallest, largest):
    def one(axis_at, parts):
        heights = jax.random.uniform(jax.random.fold_in(jax.random.fold_in(own_key, 6), axis_at), (parts,), jnp.float32, smallest / len(shards), largest / len(shards))
        return jnp.repeat(jnp.exp(heights), dims[axis_at] // parts).reshape((-1,) + (1,) * (len(dims) - axis_at - 1))

    loudness = one(*shards[0])
    for cut in shards[1:]:
        loudness = loudness * one(*cut)
    return loudness


def normal_values(own_key, shape, width, limit, cuts=(), kind=jnp.bfloat16):
    loudness = steps_of(own_key, shape, cuts, -0.22, 0.18) if cuts else 1.0
    values = jax.random.normal(own_key, shape, jnp.float32) * width * loudness
    return jnp.minimum(jnp.maximum(values, -limit), limit).astype(kind)


def gaussian_with(rng, dims, scale, reach, cuts, heavy, kind=jnp.bfloat16):
    values = scale * jax.random.normal(rng, dims, jnp.float32)
    if cuts:
        values = values * steps_of(rng, dims, cuts, -0.22, 0.18)
    return jnp.clip(strengthened(values, jax.random.fold_in(rng, 3), *heavy), -reach, reach).astype(kind)


def setup_inputs(seed: int = 0) -> dict:
    splits = jax.random.split(jax.random.key(seed), 13)
    return {
        "item_ids": draw_item_ids(jax.random.fold_in(splits[12], 71), 0),
        "table_ids": draw_table_ids(jax.random.fold_in(splits[12], 71), 0),
        "lengths": draw_lengths(jax.random.fold_in(splits[12], 71), 0),
        "assignment": draw_assignment(jax.random.fold_in(splits[12], 71), 0),
        "table_a": normal_values(splits[4], (TROWS_A, WIDTH_A), 1.0, 6.0, ((0, 256),)),
        "table_b": normal_values(splits[5], (TROWS_B, WIDTH_B), 1.0, 6.0, ((0, 256),)),
        "table_c": normal_values(splits[6], (TROWS_C, WIDTH_C), 1.0, 6.0, ((0, 256),)),
        "table_d": normal_values(splits[7], (TROWS_D, WIDTH_D), 1.0, 6.0, ((0, 256),)),
        "proj_weight": normal_values(splits[8], (WSUM, D), (WSUM // 4) ** -0.5, 0.5, ((0, 32),)),
        "in_weight": normal_values(splits[9], (D, FF), D ** -0.5, 0.25, ((0, 32),)),
        "out_weight": normal_values(splits[10], (D, D), D ** -0.5, 0.25, ((0, 32),)),
        "cotangent": gaussian_with(splits[11], (SEQS, MAXLEN, D), 1.0, 24.0, ((0, 256),), (0, 2, 256, 6.0)),
    }


def normalize(values):
    centred = values - lax.optimization_barrier(jnp.mean(values, axis=-1, keepdims=True))
    return centred * lax.rsqrt(lax.optimization_barrier(jnp.mean(centred * centred, axis=-1, keepdims=True)) + 1e-05)

def hstu_layer(embedded, seq_lengths, in_full, out_full):
    seq_count, seq_span, model_width = embedded.shape
    head_dim = model_width // HEADS
    normed = normalize(embedded.astype(jnp.float32)).astype(jnp.bfloat16)
    projected = jnp.dot(normed.reshape(seq_count * seq_span, model_width), in_full, preferred_element_type=jnp.float32)
    activated = jax.nn.silu(projected).astype(jnp.bfloat16).reshape(seq_count, seq_span, 4, HEADS, head_dim)
    gate_part = activated[:, :, 0].reshape(seq_count, seq_span, model_width)
    value_part = activated[:, :, 1].astype(jnp.float32)
    query_part = activated[:, :, 2].astype(jnp.float32)
    key_part = activated[:, :, 3].astype(jnp.float32)
    scores = jnp.einsum('sihe,sjhe->shij', query_part, key_part) * head_dim ** (-0.5)
    position = jnp.arange(seq_span, dtype=jnp.int32)
    causal = (position[None, :] <= position[:, None])[None, None]
    inside = position[None, None, None, :] < seq_lengths[:, None, None, None]
    attn = jnp.where(causal & inside, jax.nn.silu(scores), 0.0).astype(jnp.bfloat16)
    attended = jnp.einsum('shij,sjhe->sihe', attn.astype(jnp.float32), value_part).reshape(seq_count, seq_span, model_width)
    gated_rows = (normalize(attended) * gate_part.astype(jnp.float32)).astype(jnp.bfloat16)
    branch = jnp.dot(gated_rows.reshape(seq_count * seq_span, model_width), out_full, preferred_element_type=jnp.float32)
    return (embedded.astype(jnp.float32) + branch.reshape(seq_count, seq_span, model_width)).astype(jnp.bfloat16)

def reference(item_ids, table_ids, lengths, assignment, table_a, table_b, table_c, table_d, proj_weight, in_weight, out_weight, cotangent):
    tables = (table_a, table_b, table_c, table_d)
    event_items = jnp.zeros_like(item_ids).at[assignment].set(item_ids).reshape(-1)
    event_tables = jnp.zeros_like(table_ids).at[assignment].set(table_ids).reshape(-1)
    seq_lengths = jnp.zeros_like(lengths).at[assignment].set(lengths)
    pieces = []
    for which in range(4):
        hit = event_tables == which
        fetched = tables[which][jnp.where(hit, event_items, 0)]
        pieces.append(jnp.where(hit[:, None], fetched, jnp.zeros((), jnp.bfloat16)))
    rows_cat = jnp.concatenate(pieces, axis=1)
    model_width = proj_weight.shape[1]
    embedded = jnp.dot(rows_cat, proj_weight, preferred_element_type=jnp.float32).astype(jnp.bfloat16)
    embedded = embedded.reshape(DEVICES, SEQ_DEV, MAXLEN, model_width)
    position = jnp.arange(MAXLEN, dtype=jnp.int32)
    valid = position[None, :] < seq_lengths[:, None]
    out_grad = jnp.where(valid[:, :, None], cotangent, jnp.zeros((), jnp.bfloat16)).reshape(DEVICES, SEQ_DEV, MAXLEN, model_width)
    block_lengths = seq_lengths.reshape(DEVICES, SEQ_DEV)

    def step(totals, block_data):
        embed_block, length_block, grad_block = block_data

        def apply_layer(values, first_weight, second_weight):
            return hstu_layer(values, length_block, first_weight, second_weight)
        result, backward = jax.vjp(apply_layer, embed_block, in_weight, out_weight)
        d_values, d_first, d_second = backward(grad_block)
        return ((totals[0] + d_first.astype(jnp.float32), totals[1] + d_second.astype(jnp.float32)), (result, d_values))
    start = (jnp.zeros(in_weight.shape, jnp.float32), jnp.zeros(out_weight.shape, jnp.float32))
    (grad_in, grad_out), (results, d_embedded) = lax.scan(step, start, (embedded, block_lengths, out_grad))
    output = results.reshape(DEVICES * SEQ_DEV, MAXLEN, model_width)
    d_flat = d_embedded.reshape(-1, model_width)
    d_rows = jnp.dot(d_flat, proj_weight.T, preferred_element_type=jnp.float32)
    grad_proj = jnp.dot(rows_cat.T, d_flat, preferred_element_type=jnp.float32)
    table_grads = []
    column = 0
    for which in range(4):
        row_total, row_width = tables[which].shape
        target = jnp.where(event_tables == which, event_items, row_total)
        summed = jnp.zeros((row_total, row_width), jnp.float32).at[target].add(d_rows[:, column:column + row_width], mode='drop')
        table_grads.append(summed.astype(jnp.bfloat16))
        column = column + row_width
    return (output, table_grads[0], table_grads[1], table_grads[2], table_grads[3], grad_proj, grad_in, grad_out)
```

```python
import functools

import jax
import jax.numpy as jnp
from jax import lax
from jax.experimental import pallas as pl
from jax.experimental.pallas import tpu as pltpu
from jax.sharding import PartitionSpec as P

MESH = pl.DeviceIdType.MESH
VM = pl.BlockSpec(memory_space=pltpu.VMEM)
F32, BF16, I32 = jnp.float32, jnp.bfloat16, jnp.int32
NX, NY, NZ, PLANE = 4, 4, 8, 16
DEVICES = 256
HEADS, HEAD = 4, 128
SPAN, TOKENS, WIDTH = 384, 768, 512
ROWS = (12288, 12288, 6144, 2048)
FOLD = (4, 4, 2, 1)
TABLE_BITS = 22
KEY = 1024
NONE = 16383.0 * KEY
VMEM_LIMIT = 60 << 20


def place():
    dp, z = lax.axis_index("dp"), lax.axis_index("table")
    return dp, dp // 2, lax.rem(dp, 2), z


def plane_peer(xy, k):
    x = lax.rem(xy // NY + k // NY, NX)
    y = lax.rem(lax.rem(xy, NY) + k % NY, NY)
    return x * NY + y


def peers():
    dp, xy, core, z = place()
    along_z = [(dp, lax.rem(z + k, NZ)) for k in range(1, NZ)]
    in_plane = [(plane_peer(xy, k) * 2 + core, z) for k in range(1, PLANE)]
    return along_z, in_plane, [(xy * 2 + (1 - core), z)]


def near():
    dp, xy, core, z = place()
    x, y = xy // NY, lax.rem(xy, NY)
    right, left = lax.rem(x + 1, NX), lax.rem(x + NX - 1, NX)
    up, down = lax.rem(y + 1, NY), lax.rem(y + NY - 1, NY)

    def at(px, py):
        return ((px * NY + py) * 2 + core, z)

    return (x, right, left, at(right, y), at(left, y)), (y, up, down, at(x, up), at(x, down))


def greet(targets):
    barrier = pltpu.get_barrier_semaphore()
    for dp, z in targets:
        pl.semaphore_signal(barrier, inc=1, device_id=(dp, z), device_id_type=MESH)
    pl.semaphore_wait(barrier, len(targets))


def send(src, dst, send_sem, recv_sem, target):
    copy = pltpu.make_async_remote_copy(
        src_ref=src,
        dst_ref=dst,
        send_sem=send_sem,
        recv_sem=recv_sem,
        device_id=target,
        device_id_type=MESH,
    )
    copy.start()
    return copy


def dot(a, b, da=1, db=0):
    return lax.dot_general(a, b, (((da,), (db,)), ((), ())), preferred_element_type=F32)


def share_kernel(x_ref, w_ref, ids_ref, full_ref, send_sem, recv_sem, own_sem):
    dp, xy, core, z = place()
    (x, right, left, to_right, to_left), (y, up, down, to_up, to_down) = near()
    own = [
        pltpu.make_async_copy(x_ref, ids_ref.at[x, y, core, z], own_sem.at[0]),
        pltpu.make_async_copy(w_ref, full_ref.at[x, y, core], own_sem.at[1]),
    ]
    for copy in own:
        copy.start()
    along_z, _plane, partner = peers()
    greet(along_z + [to_right, to_left, to_up, to_down] + partner)
    used = [0]

    def start(src, dst, target):
        at = used[0]
        used[0] += 1
        return send(src, dst, send_sem.at[at], recv_sem.at[at], target)

    def move(ref, target):
        return start(ref, ref, target)

    def finish(copies):
        for copy in copies:
            copy.wait()

    def w(px, py, part):
        return full_ref.at[px, py, core, part]

    def ids(px, py, low, count):
        return ids_ref.at[px, py, core, pl.ds(low, count)]

    every, low, high = slice(None), pl.ds(0, 2), pl.ds(2, 2)
    first = [start(x_ref, ids_ref.at[x, y, core, z], t) for t in along_z]
    w_one = [
        start(w_ref.at[0], w(x, y, 0), to_up),
        start(w_ref.at[0], w(x, y, 0), to_down),
        start(w_ref.at[1], w(x, y, 1), to_right),
        start(w_ref.at[1], w(x, y, 1), to_left),
    ]
    finish(own + w_one)
    ahead, behind = pl.ds(0, 1536), pl.ds(1536, 1536)
    w_two = [
        move(full_ref.at[x, down, core, 0, :, ahead], to_up),
        move(full_ref.at[x, up, core, 0, :, behind], to_down),
        move(full_ref.at[left, y, core, 1, :, ahead], to_right),
        move(full_ref.at[right, y, core, 1, :, behind], to_left),
    ]
    finish(first)
    i_one = [
        move(ids(x, y, 0, 4), to_up),
        move(ids(x, y, 0, 4), to_down),
        move(ids(x, y, 4, 4), to_right),
        move(ids(x, y, 4, 4), to_left),
    ]
    finish(w_two)
    w_three = [
        move(w(x, every, 0), to_right),
        move(w(x, every, 0), to_left),
        move(w(every, y, 1), to_up),
        move(w(every, y, 1), to_down),
    ]
    finish(i_one)
    i_two = [
        move(ids(x, down, 0, 2), to_up),
        move(ids(x, up, 2, 2), to_down),
        move(ids(left, y, 4, 2), to_right),
        move(ids(right, y, 6, 2), to_left),
    ]
    finish(i_two)
    i_three = [
        move(ids(x, every, 0, 4), to_right),
        move(ids(x, every, 0, 4), to_left),
        move(ids(every, y, 4, 4), to_up),
        move(ids(every, y, 4, 4), to_down),
    ]
    finish(w_three)
    w_four = [
        move(w(left, low, 0), to_right),
        move(w(right, high, 0), to_left),
        move(w(low, down, 1), to_up),
        move(w(high, up, 1), to_down),
    ]
    finish(i_three)
    i_four = [
        move(ids(left, low, 0, 4), to_right),
        move(ids(right, high, 0, 4), to_left),
        move(ids(low, down, 4, 4), to_up),
        move(ids(high, up, 4, 4), to_down),
    ]
    finish(w_four)
    last = [move(full_ref.at[:, :, core], partner[0])]
    finish(i_four)
    last.append(move(ids_ref.at[:, :, core], partner[0]))
    finish(last)


def share(words, weights):
    columns = weights.shape[-1]
    return pl.pallas_call(
        share_kernel,
        out_shape=(
            jax.ShapeDtypeStruct((NX, NY, 2, NZ, 8, 128), I32),
            jax.ShapeDtypeStruct((NX, NY, 2, 2, 8, columns), BF16),
        ),
        in_specs=[VM, VM],
        out_specs=(VM, VM),
        scratch_shapes=[
            pltpu.SemaphoreType.DMA((41,)),
            pltpu.SemaphoreType.DMA((41,)),
            pltpu.SemaphoreType.DMA((2,)),
        ],
        compiler_params=pltpu.CompilerParams(
            collective_id=1, has_side_effects=True, vmem_limit_bytes=VMEM_LIMIT
        ),
        name="share",
    )(words, weights)


def swap_kernel(x_ref, out_ref, by_z, from_z, by_dp, from_dp, again_dp, again_z, final_z, send_sem, recv_sem):
    dp, xy, core, z = place()
    along_z, in_plane, partner = peers()
    others = [(plane_peer(xy, k) * 2 + (1 - core), z) for k in range(1, PLANE)]
    along_dp = in_plane + partner + others
    greet(along_z + along_dp)
    i = lax.broadcasted_iota(I32, (DEVICES, DEVICES), 0)
    j = lax.broadcasted_iota(I32, (DEVICES, DEVICES), 1)
    z_first = (j == (i & 31) * 8 + (i >> 5)).astype(BF16)
    dp_first = (j == (i & 7) * 32 + (i >> 3)).astype(BF16)

    def arrange(matrix, ref, dims):
        return dot(matrix, ref.reshape(DEVICES, 512)).astype(BF16).reshape(dims)

    by_dp[...] = x_ref[:, 512:1024].reshape(32, 8, 512)
    low = [
        send(by_dp.at[t[0]], from_dp.at[dp], send_sem.at[n], recv_sem.at[n], t)
        for n, t in enumerate(along_dp)
    ]
    by_z[...] = arrange(z_first, x_ref[:, 0:512], (8, 32, 512))
    high = [
        send(by_z.at[t[1]], from_z.at[z], send_sem.at[31 + n], recv_sem.at[31 + n], t)
        for n, t in enumerate(along_z)
    ]
    from_dp[pl.ds(dp, 1)] = by_dp[pl.ds(dp, 1)]
    from_z[pl.ds(z, 1)] = by_z[pl.ds(z, 1)]
    for copy in low:
        copy.wait()
    again_z[...] = arrange(z_first, from_dp[...], (8, 32, 512))
    low = [
        send(again_z.at[t[1]], final_z.at[z], send_sem.at[38 + n], recv_sem.at[38 + n], t)
        for n, t in enumerate(along_z)
    ]
    final_z[pl.ds(z, 1)] = again_z[pl.ds(z, 1)]
    for copy in high:
        copy.wait()
    again_dp[...] = arrange(dp_first, from_z[...], (32, 8, 512))
    high = [
        send(again_dp.at[t[0]], out_ref.at[0, dp], send_sem.at[45 + n], recv_sem.at[45 + n], t)
        for n, t in enumerate(along_dp)
    ]
    out_ref[0, pl.ds(dp, 1)] = again_dp[pl.ds(dp, 1)]
    for copy in low:
        copy.wait()
    out_ref[1] = arrange(dp_first, final_z[...], (32, 8, 512))
    for copy in high:
        copy.wait()


def swap(rows):
    return pl.pallas_call(
        swap_kernel,
        out_shape=jax.ShapeDtypeStruct((2, 32, 8, 512), BF16),
        in_specs=[VM],
        out_specs=VM,
        scratch_shapes=[
            pltpu.VMEM((8, 32, 512), BF16),
            pltpu.VMEM((8, 32, 512), BF16),
            pltpu.VMEM((32, 8, 512), BF16),
            pltpu.VMEM((32, 8, 512), BF16),
            pltpu.VMEM((32, 8, 512), BF16),
            pltpu.VMEM((8, 32, 512), BF16),
            pltpu.VMEM((8, 32, 512), BF16),
            pltpu.SemaphoreType.DMA((76,)),
            pltpu.SemaphoreType.DMA((76,)),
        ],
        compiler_params=pltpu.CompilerParams(
            collective_id=2, has_side_effects=True, vmem_limit_bytes=VMEM_LIMIT
        ),
        name="swap",
    )(rows)


def smallest_two(keys):
    first = jnp.full((8, keys.shape[1]), NONE, F32)
    second = first
    for at in range(0, keys.shape[0], 8):
        value = keys[at : at + 8]
        second = jnp.minimum(second, jnp.maximum(first, value))
        first = jnp.minimum(first, value)
    low = jnp.min(first, axis=0, keepdims=True)
    high = jnp.min(jnp.where(first == low, second, first), axis=0, keepdims=True)
    return low, high


def lookup_kernel(me_ref, ids_ref, a_ref, b_ref, c_ref, d_ref, send_ref, wanted_ref, cols_ref, moved):
    me = me_ref[0]
    words = jnp.concatenate(
        [
            jnp.concatenate([ids_ref[:, 4 * s + r, :] for r in range(3)], axis=1)
            for s in range(2)
        ],
        axis=0,
    )
    extra = jnp.concatenate([ids_ref[:, 3, :], ids_ref[:, 7, :]], axis=0)
    lengths = extra[:, 0:1].astype(F32)
    targets = extra[:, 1:2]
    arranged = (targets & 1) * DEVICES + (targets >> 1)
    slots = lax.broadcasted_iota(I32, (512, 512), 1)
    goes = (arranged == slots).astype(BF16)
    total = None
    for shift in (16, 8, 0):
        part = ((words >> shift) & 255).astype(F32).astype(BF16)
        piece = dot(part, goes, 0, 0)
        total = piece if total is None else total * 256.0 + piece
    moved[...] = total

    place_of = lax.broadcasted_iota(I32, (SPAN, 512), 0).astype(F32)
    lows, highs = [], []
    for which in range(4):
        start = which * (1 << TABLE_BITS) + me * ROWS[which]
        local = moved[...] - start.astype(F32)
        held = (local >= 0.0) & (local < float(ROWS[which]))
        keys = jnp.where(held, local * float(KEY) + place_of, NONE)
        low, high = smallest_two(keys)
        low_a, high_a = low[:, :DEVICES], high[:, :DEVICES]
        low_b, high_b = low[:, DEVICES:] + float(SPAN), high[:, DEVICES:] + float(SPAN)
        lows.append(jnp.minimum(low_a, low_b))
        highs.append(jnp.minimum(jnp.maximum(low_a, low_b), jnp.minimum(high_a, high_b)))
    row_form = jnp.floor(jnp.concatenate(lows + highs, axis=0) * (1.0 / KEY))
    wanted_ref[...] = row_form
    padded = jnp.concatenate([row_form, jnp.zeros((120, DEVICES), F32)], axis=0)
    col_form = jnp.transpose(padded)

    for which, table_ref in enumerate((a_ref, b_ref, c_ref, d_ref)):
        fold, rows = FOLD[which], ROWS[which]
        deep = rows // fold
        width = 256 // fold
        for rank in range(2):
            row = col_form[:, rank * 4 + which : rank * 4 + which + 1].astype(I32)
            block = row // deep
            inner = row - block * deep
            acc = jnp.zeros((DEVICES, 256), F32)
            tile = 1024
            for at in range(0, deep, tile):
                index = lax.broadcasted_iota(I32, (DEVICES, tile), 1) + at
                hot = (inner == index).astype(BF16)
                if which < 2:
                    piece = jnp.concatenate(
                        [table_ref[:, q * deep + at : q * deep + at + tile] for q in range(fold)],
                        axis=0,
                    )
                    acc = acc + dot(hot, piece, 1, 1)
                else:
                    piece = jnp.concatenate(
                        [table_ref[q * deep + at : q * deep + at + tile, :] for q in range(fold)],
                        axis=1,
                    )
                    acc = acc + dot(hot, piece)
            value = jnp.zeros((DEVICES, width), F32)
            for q in range(fold):
                value = value + jnp.where(block == q, acc[:, q * width : (q + 1) * width], 0.0)
            at = (0, 64, 256, 512)[which] + rank * (128, 128, 128, 256)[which]
            send_ref[:, at : at + width] = value.astype(BF16)

    pieces, spans = [], []
    for s in range(2):
        hit = targets == 2 * me + s
        pieces.append(jnp.sum(jnp.where(hit, words, 0), axis=0, keepdims=True))
        length = jnp.sum(jnp.where(hit, lengths, 0.0), axis=0, keepdims=True)
        spans.append(jnp.broadcast_to(length, (1, SPAN)))
    event = jnp.concatenate(pieces, axis=1)
    span = jnp.concatenate(spans, axis=1)
    table = event >> TABLE_BITS
    item = event & ((1 << TABLE_BITS) - 1)
    unit = jnp.where(table == 3, item >> 11, jnp.where(table == 2, item >> 11, item >> 12))
    third = jnp.floor((unit.astype(F32) + 0.5) * (1.0 / 3.0)).astype(I32)
    owner = jnp.where(table == 3, unit, third)
    per = jnp.where(table == 3, ROWS[3], jnp.where(table == 2, ROWS[2], ROWS[0]))
    local = item - owner * per
    order = lax.broadcasted_iota(I32, (1, TOKENS), 1)
    key = (local * KEY + order).astype(F32)
    bucket = (table * DEVICES + owner).astype(F32)
    lines = [owner.astype(F32), table.astype(F32), span, key, bucket]
    stacked = jnp.concatenate(lines + [jnp.zeros((123, TOKENS), F32)], axis=0)
    cols = jnp.transpose(stacked)
    ahead = (cols[:, 4:5] == bucket) & (key < cols[:, 3:4])
    rank = jnp.sum(jnp.where(ahead, 1.0, 0.0), axis=1, keepdims=True)
    lane = lax.broadcasted_iota(I32, (TOKENS, 128), 1)
    cols_ref[...] = jnp.where(lane == 3, rank, cols)


def lookup(me, ids, tables):
    return pl.pallas_call(
        lookup_kernel,
        out_shape=(
            jax.ShapeDtypeStruct((DEVICES, 1024), BF16),
            jax.ShapeDtypeStruct((8, DEVICES), F32),
            jax.ShapeDtypeStruct((TOKENS, 128), F32),
        ),
        in_specs=[pl.BlockSpec(memory_space=pltpu.SMEM)] + [VM] * 5,
        out_specs=(VM, VM, VM),
        scratch_shapes=[pltpu.VMEM((SPAN, 512), F32)],
        compiler_params=pltpu.CompilerParams(vmem_limit_bytes=VMEM_LIMIT),
        name="lookup",
    )(me, ids, *tables)


def moments(values):
    mean = jnp.mean(values, axis=-1, keepdims=True)
    centred = values - mean
    scale = lax.rsqrt(jnp.mean(centred * centred, axis=-1, keepdims=True) + 1e-05)
    return centred * scale, scale


def norm_back(grad, normed, scale):
    inner = jnp.mean(grad * normed, axis=-1, keepdims=True)
    return scale * (grad - jnp.mean(grad, axis=-1, keepdims=True) - normed * inner)


def sigmoid(values):
    return 0.5 * jnp.tanh(0.5 * values) + 0.5


def layer_kernel(
    got_ref, cols_ref, w_ref, cot_ref, out_ref, back_ref, g_ref,
    rows_s, emb_s, norm_s, pre_s, act_s, att_s, gated_s, dact_s, datt_s, dpre_s, demb_s, place_s,
):
    half = 128
    proj = w_ref[:, 0:512]
    out_w = w_ref[:, 2560:3072]

    def begin(s, _):
        at = pl.ds(pl.multiple_of(s * SPAN, SPAN), SPAN)
        owner = cols_ref[at, 0:1].astype(I32)
        table = cols_ref[at, 1:2]
        rank = cols_ref[at, 3:4]
        hot = (owner == lax.broadcasted_iota(I32, (SPAN, DEVICES), 1)).astype(BF16)
        lane = lax.broadcasted_iota(I32, (SPAN, half), 1)
        kind = jnp.where(lane < 64, 0.0, 1.0)
        got = dot(hot, got_ref[0])
        first = rank == 0.0
        ab = jnp.where((table == kind), jnp.where(first, got[:, 0:128], got[:, 128:256]), 0.0)
        c = jnp.where(table == 2.0, jnp.where(first, got[:, 256:384], got[:, 384:512]), 0.0)
        got = dot(hot, got_ref[1])
        d = jnp.where(table == 3.0, jnp.where(first, got[:, 0:256], got[:, 256:512]), 0.0)
        rows = jnp.concatenate([ab, c, d], axis=1).astype(BF16)
        rows_s[at, :] = rows
        emb = dot(rows, proj).astype(BF16)
        emb_s[at, :] = emb
        normed, _scale = moments(emb.astype(F32))
        norm_s[at, :] = normed.astype(BF16)
        return 0

    lax.fori_loop(0, 2, begin, 0)

    def project(i, _):
        s, part = i // 4, lax.rem(i, 4)
        at = pl.ds(pl.multiple_of(s * SPAN, SPAN), SPAN)
        lanes = pl.ds(pl.multiple_of(part * 512, 512), 512)
        pre = dot(norm_s[at, :], w_ref[:, pl.ds(pl.multiple_of(part * 512 + 512, 512), 512)])
        pre_s[at, lanes] = pre
        act_s[at, lanes] = (pre * sigmoid(pre)).astype(BF16)
        return 0

    lax.fori_loop(0, 8, project, 0)

    row_id = lax.broadcasted_iota(I32, (SPAN, SPAN), 0)
    col_id = lax.broadcasted_iota(I32, (SPAN, SPAN), 1)

    def head_lanes(kind, head):
        return pl.ds(pl.multiple_of(kind * 512 + head * HEAD, HEAD), HEAD)

    def attend(i, _):
        s, head = i // 4, lax.rem(i, 4)
        at = pl.ds(pl.multiple_of(s * SPAN, SPAN), SPAN)
        keep = (col_id <= row_id) & (col_id.astype(F32) < cols_ref[at, 2:3])
        value = act_s[at, head_lanes(1, head)]
        query = act_s[at, head_lanes(2, head)]
        key = act_s[at, head_lanes(3, head)]
        scores = dot(query, key, 1, 1) * HEAD**-0.5
        attn = jnp.where(keep, scores * sigmoid(scores), 0.0).astype(BF16)
        att_s[at, head_lanes(0, head)] = dot(attn, value)
        return 0

    lax.fori_loop(0, 8, attend, 0)

    def middle(s, _):
        at = pl.ds(pl.multiple_of(s * SPAN, SPAN), SPAN)
        normed, scale = moments(att_s[at, :])
        gate = act_s[at, 0:512].astype(F32)
        gated = (normed * gate).astype(BF16)
        gated_s[at, :] = gated
        branch = dot(gated, out_w)
        out_ref[at, :] = (emb_s[at, :].astype(F32) + branch).astype(BF16)
        where = lax.broadcasted_iota(I32, (SPAN, 1), 0).astype(F32)
        grad = jnp.where(where < cols_ref[at, 2:3], cot_ref[at, :], jnp.zeros((), BF16))
        demb_s[at, :] = grad
        d_gated = dot(grad, out_w, 1, 1).astype(BF16).astype(F32)
        dact_s[at, 0:512] = (d_gated * normed).astype(BF16)
        datt_s[at, :] = norm_back(d_gated * gate, normed, scale).astype(BF16)
        return 0

    lax.fori_loop(0, 2, middle, 0)
    g_ref[:, 2560:3072] = dot(gated_s[...], demb_s[...], 0, 0).astype(BF16)

    def attend_back(i, _):
        s, head = i // 4, lax.rem(i, 4)
        at = pl.ds(pl.multiple_of(s * SPAN, SPAN), SPAN)
        keep = (col_id <= row_id) & (col_id.astype(F32) < cols_ref[at, 2:3])
        value = act_s[at, head_lanes(1, head)]
        query = act_s[at, head_lanes(2, head)]
        key = act_s[at, head_lanes(3, head)]
        d_att = datt_s[at, head_lanes(0, head)]
        scores = dot(query, key, 1, 1) * HEAD**-0.5
        sig = sigmoid(scores)
        attn = jnp.where(keep, scores * sig, 0.0).astype(BF16)
        d_attn = dot(d_att, value, 1, 1).astype(BF16).astype(F32)
        slope = sig * (1.0 + scores * (1.0 - sig))
        d_scores = (jnp.where(keep, d_attn * slope, 0.0) * HEAD**-0.5).astype(BF16)
        dact_s[at, head_lanes(1, head)] = dot(attn, d_att, 0, 0).astype(BF16)
        dact_s[at, head_lanes(2, head)] = dot(d_scores, key).astype(BF16)
        dact_s[at, head_lanes(3, head)] = dot(d_scores, query, 0, 0).astype(BF16)
        return 0

    lax.fori_loop(0, 8, attend_back, 0)

    def project_back(i, _):
        s, part = i // 4, lax.rem(i, 4)
        at = pl.ds(pl.multiple_of(s * SPAN, SPAN), SPAN)
        lanes = pl.ds(pl.multiple_of(part * 512, 512), 512)
        pre = pre_s[at, lanes]
        sig = sigmoid(pre)
        slope = sig * (1.0 + pre * (1.0 - sig))
        dpre_s[at, lanes] = (dact_s[at, lanes].astype(F32) * slope).astype(BF16)
        return 0

    lax.fori_loop(0, 8, project_back, 0)

    def first_weight(part, _):
        lanes = pl.ds(pl.multiple_of(part * 512, 512), 512)
        wide = pl.ds(pl.multiple_of(part * 512 + 512, 512), 512)
        g_ref[:, wide] = dot(norm_s[...], dpre_s[:, lanes], 0, 0).astype(BF16)
        return 0

    lax.fori_loop(0, 4, first_weight, 0)

    def finish(s, _):
        at = pl.ds(pl.multiple_of(s * SPAN, SPAN), SPAN)
        d_normed = dot(dpre_s[at, 0:512], w_ref[:, 512:1024], 1, 1)
        for part in range(1, 4):
            lanes = slice(part * 512, part * 512 + 512)
            wide = slice(part * 512 + 512, part * 512 + 1024)
            d_normed = d_normed + dot(dpre_s[at, lanes], w_ref[:, wide], 1, 1)
        normed, scale = moments(emb_s[at, :].astype(F32))
        back = norm_back(d_normed.astype(BF16).astype(F32), normed, scale)
        d_emb = (demb_s[at, :].astype(F32) + back).astype(BF16)
        demb_s[at, :] = d_emb
        d_rows = dot(d_emb, proj, 1, 1)
        table = cols_ref[at, 1:2]
        rank = cols_ref[at, 3:4]
        lane = lax.broadcasted_iota(I32, (SPAN, half), 1)
        kind = jnp.where(lane < 64, 0.0, 1.0)
        for k in range(2):
            match = rank == float(k)
            low = k * 128
            place_s[at, low : low + 128] = jnp.where(
                (table == kind) & match, d_rows[:, 0:128], 0.0
            ).astype(BF16)
            place_s[at, 256 + low : 384 + low] = jnp.where(
                (table == 2.0) & match, d_rows[:, 128:256], 0.0
            ).astype(BF16)
            low = 512 + k * 256
            place_s[at, low : low + 256] = jnp.where(
                (table == 3.0) & match, d_rows[:, 256:512], 0.0
            ).astype(BF16)
        return 0

    lax.fori_loop(0, 2, finish, 0)
    g_ref[:, 0:512] = dot(rows_s[...], demb_s[...], 0, 0).astype(BF16)
    owner = cols_ref[:, 0:1].astype(I32)
    hot = (owner == lax.broadcasted_iota(I32, (TOKENS, DEVICES), 1)).astype(BF16)
    for part in range(2):
        lanes = slice(part * 512, part * 512 + 512)
        back_ref[:, lanes] = dot(hot, place_s[:, lanes], 0, 0).astype(BF16)


def layer(got, cols, weights, cotangent):
    def vmem(width, kind=BF16):
        return pltpu.VMEM((TOKENS, width), kind)

    return pl.pallas_call(
        layer_kernel,
        out_shape=(
            jax.ShapeDtypeStruct((TOKENS, WIDTH), BF16),
            jax.ShapeDtypeStruct((DEVICES, 1024), BF16),
            jax.ShapeDtypeStruct((512, 3072), BF16),
        ),
        in_specs=[VM] * 4,
        out_specs=(VM, VM, VM),
        scratch_shapes=[
            vmem(512), vmem(512), vmem(512), vmem(2048, F32), vmem(2048), vmem(512, F32),
            vmem(512), vmem(2048), vmem(512), vmem(2048), vmem(512), vmem(1024),
        ],
        compiler_params=pltpu.CompilerParams(vmem_limit_bytes=VMEM_LIMIT),
        name="layer",
    )(got, cols, weights, cotangent)


def scatter_kernel(got_ref, wanted_ref, a_ref, b_ref, c_ref, d_ref):
    row_form = wanted_ref[...]
    padded = jnp.concatenate([row_form, jnp.zeros((120, DEVICES), F32)], axis=0)
    col_form = jnp.transpose(padded)
    for which, out_ref in enumerate((a_ref, b_ref, c_ref, d_ref)):
        fold, rows = FOLD[which], ROWS[which]
        deep = rows // fold
        width = 256 // fold
        spread, inners = [], []
        for rank in range(2):
            row = col_form[:, rank * 4 + which : rank * 4 + which + 1].astype(I32)
            block = row // deep
            at = (0, 64, 256, 512)[which] + rank * (128, 128, 128, 256)[which]
            value = got_ref[:, at : at + width].astype(F32)
            spread.append(
                jnp.concatenate([jnp.where(block == q, value, 0.0) for q in range(fold)], axis=1)
            )
            if which < 2:
                inners.append(row - block * deep)
            else:
                line = row_form[rank * 4 + which : rank * 4 + which + 1].astype(I32)
                inners.append(line - (line // deep) * deep)
        values = jnp.concatenate(spread, axis=0).astype(BF16)
        if which < 2:
            inner = jnp.concatenate(inners, axis=0)
            flipped = jnp.transpose(values.astype(F32)).astype(BF16)
            for at in range(0, deep, 512):
                hot = (inner == lax.broadcasted_iota(I32, (512, 512), 1) + at).astype(BF16)
                summed = dot(flipped, hot).astype(BF16)
                for q in range(fold):
                    out_ref[:, q * deep + at : q * deep + at + 512] = summed[
                        q * width : (q + 1) * width
                    ]
        else:
            inner = jnp.concatenate(inners, axis=1)
            for at in range(0, deep, 512):
                hot = (inner == lax.broadcasted_iota(I32, (512, 512), 0) + at).astype(BF16)
                summed = dot(hot, values).astype(BF16)
                for q in range(fold):
                    out_ref[q * deep + at : q * deep + at + 512, :] = summed[
                        :, q * width : (q + 1) * width
                    ]


def scatter(got, wanted):
    return pl.pallas_call(
        scatter_kernel,
        out_shape=(
            jax.ShapeDtypeStruct((64, ROWS[0]), BF16),
            jax.ShapeDtypeStruct((64, ROWS[1]), BF16),
            jax.ShapeDtypeStruct((ROWS[2], 128), BF16),
            jax.ShapeDtypeStruct((ROWS[3], 256), BF16),
        ),
        in_specs=[VM, VM],
        out_specs=(VM,) * 4,
        compiler_params=pltpu.CompilerParams(vmem_limit_bytes=VMEM_LIMIT),
        name="scatter",
    )(got, wanted)


def reduce_kernel(
    g_ref, proj_ref, in_ref, out_ref,
    across, pair, one, two, line, three, four, parts, column, mine, whole, send_sem, recv_sem,
):
    dp, xy, core, z = place()
    (x, right, left, to_right, to_left), (y, up, down, to_up, to_down) = near()
    along_z, _plane, partner = peers()
    greet(along_z + [to_right, to_left, to_up, to_down] + partner)
    used = [0]

    def start(src, dst, target):
        at = used[0]
        used[0] += 1
        return send(src, dst, send_sem.at[at], recv_sem.at[at], target)

    def finish(copies):
        for copy in copies:
            copy.wait()

    def add(*values):
        total = values[0].astype(F32)
        for value in values[1:]:
            total = total + value.astype(F32)
        return total

    finish([start(g_ref.at[:, :, 1 - core], across, partner[0])])
    far_x, far_y = lax.rem(x + 2, NX), lax.rem(y + 2, NY)

    def merge(k, _):
        i, j = k // NY, lax.rem(k, NY)
        pair[i, j] = add(g_ref[i, j, core], across[i, j]).astype(BF16)
        return 0

    lax.fori_loop(0, PLANE, merge, 0)
    low, high = pl.ds(0, 2), pl.ds(2, 2)
    finish(
        [
            start(pair.at[far_x, low, 0], one.at[0], to_right),
            start(pair.at[far_x, high, 0], one.at[1], to_left),
            start(pair.at[low, far_y, 1], one.at[2], to_up),
            start(pair.at[high, far_y, 1], one.at[3], to_down),
        ]
    )
    for k in range(2):
        pair[right, k, 0] = add(pair[right, k, 0], one[0, k]).astype(BF16)
        pair[left, 2 + k, 0] = add(pair[left, 2 + k, 0], one[1, k]).astype(BF16)
        pair[k, up, 1] = add(pair[k, up, 1], one[2, k]).astype(BF16)
        pair[2 + k, down, 1] = add(pair[2 + k, down, 1], one[3, k]).astype(BF16)
    finish(
        [
            start(pair.at[right, :, 0], two.at[0], to_right),
            start(pair.at[left, :, 0], two.at[1], to_left),
            start(pair.at[:, up, 1], two.at[2], to_up),
            start(pair.at[:, down, 1], two.at[3], to_down),
        ]
    )
    for k in range(4):
        line[0, k] = add(pair[x, k, 0], two[0, k], two[1, k]).astype(BF16)
        line[1, k] = add(pair[k, y, 1], two[2, k], two[3, k]).astype(BF16)
    ahead, behind = pl.ds(0, 1536), pl.ds(1536, 1536)
    finish(
        [
            start(line.at[0, far_y, :, ahead], three.at[0], to_up),
            start(line.at[0, far_y, :, behind], three.at[1], to_down),
            start(line.at[1, far_x, :, ahead], three.at[2], to_right),
            start(line.at[1, far_x, :, behind], three.at[3], to_left),
        ]
    )
    line[0, up, :, ahead] = add(line[0, up, :, ahead], three[0]).astype(BF16)
    line[0, down, :, behind] = add(line[0, down, :, behind], three[1]).astype(BF16)
    line[1, right, :, ahead] = add(line[1, right, :, ahead], three[2]).astype(BF16)
    line[1, left, :, behind] = add(line[1, left, :, behind], three[3]).astype(BF16)
    finish(
        [
            start(line.at[0, up], four.at[0], to_up),
            start(line.at[0, down], four.at[1], to_down),
            start(line.at[1, right], four.at[2], to_right),
            start(line.at[1, left], four.at[3], to_left),
        ]
    )
    for q in range(NZ):
        lanes = pl.ds(q * 384, 384)
        parts[q, 0] = add(line[0, y, :, lanes], four[0, :, lanes], four[1, :, lanes]).astype(BF16)
        parts[q, 1] = add(line[1, x, :, lanes], four[2, :, lanes], four[3, :, lanes]).astype(BF16)
    finish([start(parts.at[t[1]], column.at[i], t) for i, t in enumerate(along_z)])
    mine[...] = add(parts[z], *[column[k] for k in range(NZ - 1)]).astype(BF16)
    copies = [start(mine, whole.at[z], t) for t in along_z]
    whole[pl.ds(z, 1)] = mine[...][None]
    finish(copies)
    for half in range(2):
        rows = slice(half * 8, half * 8 + 8)
        total = jnp.concatenate([whole[q, half].astype(F32) for q in range(NZ)], axis=1)
        proj_ref[rows, :] = total[:, 0:512]
        in_ref[rows, :] = total[:, 512:2560]
        out_ref[rows, :] = total[:, 2560:3072]


def reduce_weights(terms):
    return pl.pallas_call(
        reduce_kernel,
        out_shape=(
            jax.ShapeDtypeStruct((16, 512), F32),
            jax.ShapeDtypeStruct((16, 2048), F32),
            jax.ShapeDtypeStruct((16, 512), F32),
        ),
        in_specs=[VM],
        out_specs=(VM, VM, VM),
        scratch_shapes=[
            pltpu.VMEM((4, 4, 2, 8, 3072), BF16),
            pltpu.VMEM((4, 4, 2, 8, 3072), BF16),
            pltpu.VMEM((4, 2, 8, 3072), BF16),
            pltpu.VMEM((4, 4, 8, 3072), BF16),
            pltpu.VMEM((2, 4, 8, 3072), BF16),
            pltpu.VMEM((4, 8, 1536), BF16),
            pltpu.VMEM((4, 8, 3072), BF16),
            pltpu.VMEM((8, 2, 8, 384), BF16),
            pltpu.VMEM((7, 2, 8, 384), BF16),
            pltpu.VMEM((2, 8, 384), BF16),
            pltpu.VMEM((8, 2, 8, 384), BF16),
            pltpu.SemaphoreType.DMA((31,)),
            pltpu.SemaphoreType.DMA((31,)),
        ],
        compiler_params=pltpu.CompilerParams(
            collective_id=4, has_side_effects=True, vmem_limit_bytes=VMEM_LIMIT
        ),
        name="reduce_weights",
    )(terms)


def shards(
    item_ids, table_ids, lengths, assignment,
    table_a, table_b, table_c, table_d,
    proj_weight, in_weight, out_weight, cotangent,
):
    events = table_ids * (1 << TABLE_BITS) + item_ids
    last = jnp.concatenate(
        [lengths[:, None], assignment[:, None], jnp.zeros((2, 126), I32)], axis=1
    )
    words = jnp.concatenate([events, last], axis=1).reshape(8, 128)
    weights = jnp.concatenate([proj_weight, in_weight, out_weight], axis=1)
    ids, full = share(words, weights.reshape(2, 8, 3072))
    me = (lax.axis_index("dp") * NZ + lax.axis_index("table")).astype(I32).reshape(1)
    outgoing, wanted, cols = lookup(
        me, ids.reshape(DEVICES, 8, 128), (table_a.T, table_b.T, table_c, table_d)
    )
    got = swap(outgoing).reshape(2, DEVICES, 512)
    output, back, terms = layer(
        got, cols, full.reshape(512, 3072), cotangent.reshape(TOKENS, WIDTH)
    )
    arrived = lax.all_to_all(back, ("dp", "table"), 0, 0, tiled=True)
    totals = reduce_weights(terms.reshape(NX, NY, 2, 2, 8, 3072))
    grad_a, grad_b, grad_c, grad_d = scatter(arrived, wanted)
    return (
        output.reshape(2, SPAN, WIDTH),
        grad_a.T,
        grad_b.T,
        grad_c,
        grad_d,
        *totals,
    )


def solution(mesh):
    both = ("dp", "table")
    return jax.shard_map(
        shards,
        mesh=mesh,
        in_specs=(
            P(both, None), P(both, None), P(both), P(both),
            P(both, None), P(both, None), P(both, None), P(both, None),
            P("dp", None), P("dp", None), P("dp", None), P(both, None, None),
        ),
        out_specs=(
            P(both, None, None),
            P(both, None), P(both, None), P(both, None), P(both, None),
            P("dp", None), P("dp", None), P("dp", None),
        ),
        check_vma=False,
    )
```

```python
import functools

import jax
import jax.numpy as jnp
from jax import lax
from jax.experimental import pallas as pl
from jax.experimental.pallas import tpu as pltpu
from jax.sharding import PartitionSpec as P

MESH = pl.DeviceIdType.MESH
VM = pl.BlockSpec(memory_space=pltpu.VMEM)
F32, BF16, I32 = jnp.float32, jnp.bfloat16, jnp.int32
NX, NY, NZ, PLANE = 4, 4, 8, 16
DEVICES = 256
HEADS, HEAD = 4, 128
SPAN, TOKENS, WIDTH = 384, 768, 512
ROWS = (12288, 12288, 6144, 2048)
FOLD = (4, 4, 2, 1)
TABLE_BITS = 22
KEY = 1024
NONE = 16383.0 * KEY
VMEM_LIMIT = 60 << 20
UNROLL = 2
ANY = pl.BlockSpec(memory_space=pl.ANY)


def place():
    dp, z = lax.axis_index("dp"), lax.axis_index("table")
    return dp, dp // 2, lax.rem(dp, 2), z


def plane_peer(xy, k):
    x = lax.rem(xy // NY + k // NY, NX)
    y = lax.rem(lax.rem(xy, NY) + k % NY, NY)
    return x * NY + y


def peers():
    dp, xy, core, z = place()
    along_z = [(dp, lax.rem(z + k, NZ)) for k in range(1, NZ)]
    in_plane = [(plane_peer(xy, k) * 2 + core, z) for k in range(1, PLANE)]
    return along_z, in_plane, [(xy * 2 + (1 - core), z)]


def near():
    dp, xy, core, z = place()
    x, y = xy // NY, lax.rem(xy, NY)
    right, left = lax.rem(x + 1, NX), lax.rem(x + NX - 1, NX)
    up, down = lax.rem(y + 1, NY), lax.rem(y + NY - 1, NY)

    def at(px, py):
        return ((px * NY + py) * 2 + core, z)

    return (x, right, left, at(right, y), at(left, y)), (y, up, down, at(x, up), at(x, down))


def greet(targets):
    barrier = pltpu.get_barrier_semaphore()
    for dp, z in targets:
        pl.semaphore_signal(barrier, inc=1, device_id=(dp, z), device_id_type=MESH)
    pl.semaphore_wait(barrier, len(targets))


def send(src, dst, send_sem, recv_sem, target):
    copy = pltpu.make_async_remote_copy(
        src_ref=src,
        dst_ref=dst,
        send_sem=send_sem,
        recv_sem=recv_sem,
        device_id=target,
        device_id_type=MESH,
    )
    copy.start()
    return copy


def dot(a, b, da=1, db=0):
    return lax.dot_general(a, b, (((da,), (db,)), ((), ())), preferred_element_type=F32)


class Sender:
    def __init__(self, send_sem, recv_sem):
        self.sems, self.used = (send_sem, recv_sem), 0

    def start(self, src, dst, target):
        at, self.used = self.used, self.used + 1
        return send(src, dst, self.sems[0].at[at], self.sems[1].at[at], target)

    def move(self, ref, target):
        return self.start(ref, ref, target)


def finish(copies):
    for copy in copies:
        copy.wait()


EVERY, LOW, HIGH = slice(None), pl.ds(0, 2), pl.ds(2, 2)
AHEAD, BEHIND = pl.ds(0, 1536), pl.ds(1536, 1536)


def share_kernel(
    items_ref, tables_ref, lengths_ref, targets_ref, proj_ref, in_ref, wout_ref,
    ids_ref, full_ref, send_sem, recv_sem,
):
    dp, xy, core, z = place()
    (x, right, left, to_right, to_left), (y, up, down, to_up, to_down) = near()
    far_x, far_y = lax.rem(x + 2, NX), lax.rem(y + 2, NY)
    to_far_x, to_far_y = ((far_x * NY + y) * 2 + core, z), ((x * NY + far_y) * 2 + core, z)
    lane = lax.broadcasted_iota(I32, (1, 128), 1)
    events = tables_ref[...] * (1 << TABLE_BITS) + items_ref[...]
    lines = []
    for s in range(2):
        lines += [events[s : s + 1, r * 128 : r * 128 + 128] for r in range(3)]
        lines.append(jnp.where(lane == 0, lengths_ref[s], jnp.where(lane == 1, targets_ref[s], 0)))
    ids_ref[x, y, core, z] = jnp.concatenate(lines, axis=0)
    for half in range(2):
        rows = slice(half * 8, half * 8 + 8)
        full_ref[x, y, core, half, :, 0:512] = proj_ref[rows, :]
        full_ref[x, y, core, half, :, 512:2560] = in_ref[rows, :]
        full_ref[x, y, core, half, :, 2560:3072] = wout_ref[rows, :]
    along_z, _plane, partner = peers()
    partner = partner[0]
    near_x, near_y = [to_right, to_left], [to_up, to_down]
    greet(along_z + near_x + near_y + [to_far_x, to_far_y, partner])
    link = Sender(send_sem, recv_sem)

    def ids(px, py, low):
        return ids_ref.at[px, py, core, pl.ds(low, 4)]

    def w(px, py, part):
        return full_ref.at[px, py, core, part]

    own = ids_ref.at[x, y, core, z]
    one = [link.move(own, t) for t in along_z]
    w_one = [link.move(w(x, y, 0), t) for t in near_y] + [link.move(w(x, y, 1), t) for t in near_x]
    finish(one)
    two = [link.move(ids(x, y, 0), t) for t in near_y + [to_far_y]]
    two += [link.move(ids(x, y, 4), t) for t in near_x + [to_far_x]]
    finish(w_one)
    w_two = [
        link.move(full_ref.at[x, down, core, 0, :, AHEAD], to_up),
        link.move(full_ref.at[x, up, core, 0, :, BEHIND], to_down),
        link.move(full_ref.at[left, y, core, 1, :, AHEAD], to_right),
        link.move(full_ref.at[right, y, core, 1, :, BEHIND], to_left),
    ]
    finish(two)
    three = [link.move(ids(x, EVERY, 0), t) for t in [to_far_x] + near_x]
    three += [link.move(ids(EVERY, y, 4), t) for t in [to_far_y] + near_y]
    across = [link.move(ids(x, EVERY, 0), partner), link.move(ids(EVERY, y, 4), partner)]
    finish(w_two)
    w_three = [
        link.move(w(x, EVERY, 0), to_right),
        link.move(w(x, EVERY, 0), to_left),
        link.move(w(EVERY, y, 1), to_up),
        link.move(w(EVERY, y, 1), to_down),
    ]
    across += [link.move(w(x, EVERY, 0), partner), link.move(w(EVERY, y, 1), partner)]
    finish(three)
    across += [link.move(ids(side, EVERY, 0), partner) for side in (right, left, far_x)]
    across += [link.move(ids(EVERY, side, 4), partner) for side in (up, down, far_y)]
    finish(w_three)
    w_four = [
        link.move(w(left, LOW, 0), to_right),
        link.move(w(right, HIGH, 0), to_left),
        link.move(w(LOW, down, 1), to_up),
        link.move(w(HIGH, up, 1), to_down),
    ]
    across += [link.move(w(side, EVERY, 0), partner) for side in (right, left)]
    across += [link.move(w(EVERY, side, 1), partner) for side in (up, down)]
    finish(w_four)
    across += [link.move(w(far_x, EVERY, 0), partner), link.move(w(EVERY, far_y, 1), partner)]
    finish(across)


def sems(count):
    return [pltpu.SemaphoreType.DMA((count,)), pltpu.SemaphoreType.DMA((count,))]


def comm_params(collective):
    return pltpu.CompilerParams(
        collective_id=collective, has_side_effects=True, vmem_limit_bytes=VMEM_LIMIT
    )


SM = pl.BlockSpec(memory_space=pltpu.SMEM)


def share(items, tables, lengths, targets, weights):
    return pl.pallas_call(
        share_kernel,
        out_shape=(
            jax.ShapeDtypeStruct((NX, NY, 2, NZ, 8, 128), I32),
            jax.ShapeDtypeStruct((NX, NY, 2, 2, 8, 3072), BF16),
        ),
        in_specs=[VM, VM, SM, SM, VM, VM, VM],
        out_specs=(VM, VM),
        scratch_shapes=sems(51),
        compiler_params=comm_params(1),
        name="share",
    )(items, tables, lengths, targets, *weights)


class Swap:
    def __init__(self, link, first_ref, second_ref, out_ref, by_z, from_z, by_dp, from_dp, again_z, from_z2):
        self.link, self.first, self.second, self.out = link, first_ref, second_ref, out_ref
        self.by_z, self.from_z, self.by_dp = by_z, from_z, by_dp
        self.from_dp, self.again_z, self.from_z2 = from_dp, again_z, from_z2
        self.dp, xy, core, self.z = place()
        self.along_z, in_plane, partner = peers()
        others = [(plane_peer(xy, k) * 2 + (1 - core), self.z) for k in range(1, PLANE)]
        self.along_dp = in_plane + partner + others
        i = lax.broadcasted_iota(I32, (DEVICES, DEVICES), 0)
        j = lax.broadcasted_iota(I32, (DEVICES, DEVICES), 1)
        self.z_first = (j == (i & 31) * 8 + (i >> 5)).astype(BF16)
        self.dp_first = (j == (i & 7) * 32 + (i >> 3)).astype(BF16)
        by_z[...] = self.arrange(self.z_first, first_ref, (NZ, 32, 512))
        from_z[pl.ds(self.z, 1)] = by_z[pl.ds(self.z, 1)]
        from_dp[pl.ds(self.dp, 1)] = second_ref[pl.ds(self.dp, 1)]

    def arrange(self, matrix, ref, dims):
        return dot(matrix, ref[...].reshape(DEVICES, 512)).astype(BF16).reshape(dims)

    def begin_high(self):
        return [self.link.start(self.by_z.at[t[1]], self.from_z.at[self.z], t) for t in self.along_z]

    def begin_low(self):
        return [
            self.link.start(self.second.at[t[0]], self.from_dp.at[self.dp], t)
            for t in self.along_dp
        ]

    def turn_low(self):
        self.again_z[...] = self.arrange(self.z_first, self.from_dp, (NZ, 32, 512))
        self.from_z2[pl.ds(self.z, 1)] = self.again_z[pl.ds(self.z, 1)]
        return [
            self.link.start(self.again_z.at[t[1]], self.from_z2.at[self.z], t)
            for t in self.along_z
        ]

    def turn_high(self):
        self.by_dp[...] = self.arrange(self.dp_first, self.from_z, (32, NZ, 512))
        self.out[0, pl.ds(self.dp, 1)] = self.by_dp[pl.ds(self.dp, 1)]
        return [
            self.link.start(self.by_dp.at[t[0]], self.out.at[0, self.dp], t) for t in self.along_dp
        ]

    def end_low(self):
        self.out[1] = self.arrange(self.dp_first, self.from_z2, (32, NZ, 512))


SWAP_SHAPES = [
    pltpu.VMEM((8, 32, 512), BF16),
    pltpu.VMEM((8, 32, 512), BF16),
    pltpu.VMEM((32, 8, 512), BF16),
    pltpu.VMEM((32, 8, 512), BF16),
    pltpu.VMEM((8, 32, 512), BF16),
    pltpu.VMEM((8, 32, 512), BF16),
]


def fetch_kernel(first_ref, second_ref, out_ref, *scratch):
    swap = Swap(Sender(*scratch[-2:]), first_ref, second_ref, out_ref, *scratch[:-2])
    greet(swap.along_z + swap.along_dp)
    low, high = swap.begin_low(), swap.begin_high()
    finish(low)
    low = swap.turn_low()
    finish(high)
    high = swap.turn_high()
    finish(low)
    swap.end_low()
    finish(high)


def fetch(first, second):
    return pl.pallas_call(
        fetch_kernel,
        out_shape=jax.ShapeDtypeStruct((2, 32, 8, 512), BF16),
        in_specs=[VM] * 2,
        out_specs=VM,
        scratch_shapes=SWAP_SHAPES + sems(76),
        compiler_params=comm_params(2),
        name="fetch",
    )(first, second)


def smallest_two(keys):
    first = jnp.full((8, keys.shape[1]), NONE, F32)
    second = first
    for at in range(0, keys.shape[0], 8):
        value = keys[at : at + 8]
        second = jnp.minimum(second, jnp.maximum(first, value))
        first = jnp.minimum(first, value)
    low = jnp.min(first, axis=0, keepdims=True)
    high = jnp.min(jnp.where(first == low, second, first), axis=0, keepdims=True)
    return low, high


def lookup_kernel(
    me_ref, ids_ref, a_hbm, b_hbm, c_hbm, d_hbm, first_ref, second_ref, wanted_ref, cols_ref,
    moved, a_ref, b_ref, c_ref, d_ref, sem,
):
    hbm, tables = (a_hbm, b_hbm, c_hbm, d_hbm), (a_ref, b_ref, c_ref, d_ref)
    loads = [pltpu.make_async_copy(hbm[i], tables[i], sem.at[i]) for i in range(4)]
    for copy in loads:
        copy.start()
    me = me_ref[0]
    words = jnp.concatenate(
        [
            jnp.concatenate([ids_ref[:, 4 * s + r, :] for r in range(3)], axis=1)
            for s in range(2)
        ],
        axis=0,
    )
    extra = jnp.concatenate([ids_ref[:, 3, :], ids_ref[:, 7, :]], axis=0)
    lengths = extra[:, 0:1].astype(F32)
    targets = extra[:, 1:2]
    arranged = (targets & 1) * DEVICES + (targets >> 1)
    slots = lax.broadcasted_iota(I32, (512, 512), 1)
    goes = (arranged == slots).astype(BF16)
    total = None
    for shift in (16, 8, 0):
        part = ((words >> shift) & 255).astype(F32).astype(BF16)
        piece = dot(part, goes, 0, 0)
        total = piece if total is None else total * 256.0 + piece
    moved[...] = total

    place_of = lax.broadcasted_iota(I32, (SPAN, 512), 0).astype(F32)
    lows, highs = [], []
    for which in range(4):
        start = which * (1 << TABLE_BITS) + me * ROWS[which]
        local = moved[...] - start.astype(F32)
        held = (local >= 0.0) & (local < float(ROWS[which]))
        keys = jnp.where(held, local * float(KEY) + place_of, NONE)
        low, high = smallest_two(keys)
        low_a, high_a = low[:, :DEVICES], high[:, :DEVICES]
        low_b, high_b = low[:, DEVICES:] + float(SPAN), high[:, DEVICES:] + float(SPAN)
        lows.append(jnp.minimum(low_a, low_b))
        highs.append(jnp.minimum(jnp.maximum(low_a, low_b), jnp.minimum(high_a, high_b)))
    row_form = jnp.floor(jnp.concatenate(lows + highs, axis=0) * (1.0 / KEY))
    wanted_ref[...] = row_form
    padded = jnp.concatenate([row_form, jnp.zeros((120, DEVICES), F32)], axis=0)
    col_form = jnp.transpose(padded)

    for which, table_ref in enumerate(tables):
        loads[which].wait()
        fold, rows = FOLD[which], ROWS[which]
        deep = rows // fold
        width = 256 // fold
        for rank in range(2):
            row = col_form[:, rank * 4 + which : rank * 4 + which + 1].astype(I32)
            block = row // deep
            inner = row - block * deep
            acc = jnp.zeros((DEVICES, 256), F32)
            tile = 1024
            for at in range(0, deep, tile):
                index = lax.broadcasted_iota(I32, (DEVICES, tile), 1) + at
                hot = (inner == index).astype(BF16)
                if which < 2:
                    piece = jnp.concatenate(
                        [table_ref[:, q * deep + at : q * deep + at + tile] for q in range(fold)],
                        axis=0,
                    )
                    acc = acc + dot(hot, piece, 1, 1)
                else:
                    piece = jnp.concatenate(
                        [table_ref[q * deep + at : q * deep + at + tile, :] for q in range(fold)],
                        axis=1,
                    )
                    acc = acc + dot(hot, piece)
            value = jnp.zeros((DEVICES, width), F32)
            for q in range(fold):
                value = value + jnp.where(block == q, acc[:, q * width : (q + 1) * width], 0.0)
            at = (0, 64, 256, 0)[which] + rank * (128, 128, 128, 256)[which]
            part_ref = second_ref if which == 3 else first_ref
            part_ref[:, at : at + width] = value.astype(BF16)

    pieces, spans = [], []
    for s in range(2):
        hit = targets == 2 * me + s
        pieces.append(jnp.sum(jnp.where(hit, words, 0), axis=0, keepdims=True))
        length = jnp.sum(jnp.where(hit, lengths, 0.0), axis=0, keepdims=True)
        spans.append(jnp.broadcast_to(length, (1, SPAN)))
    event = jnp.concatenate(pieces, axis=1)
    span = jnp.concatenate(spans, axis=1)
    table = event >> TABLE_BITS
    item = event & ((1 << TABLE_BITS) - 1)
    unit = jnp.where(table == 3, item >> 11, jnp.where(table == 2, item >> 11, item >> 12))
    third = jnp.floor((unit.astype(F32) + 0.5) * (1.0 / 3.0)).astype(I32)
    owner = jnp.where(table == 3, unit, third)
    per = jnp.where(table == 3, ROWS[3], jnp.where(table == 2, ROWS[2], ROWS[0]))
    local = item - owner * per
    order = lax.broadcasted_iota(I32, (1, TOKENS), 1)
    key = (local * KEY + order).astype(F32)
    bucket = (table * DEVICES + owner).astype(F32)
    lines = [owner.astype(F32), table.astype(F32), span, key, bucket]
    stacked = jnp.concatenate(lines + [jnp.zeros((123, TOKENS), F32)], axis=0)
    cols = jnp.transpose(stacked)
    ahead = (cols[:, 4:5] == bucket) & (key < cols[:, 3:4])
    rank = jnp.sum(jnp.where(ahead, 1.0, 0.0), axis=1, keepdims=True)
    lane = lax.broadcasted_iota(I32, (TOKENS, 128), 1)
    cols_ref[...] = jnp.where(lane == 3, rank, cols)


def lookup(me, ids, tables):
    return pl.pallas_call(
        lookup_kernel,
        out_shape=(
            jax.ShapeDtypeStruct((DEVICES, 512), BF16),
            jax.ShapeDtypeStruct((DEVICES, 512), BF16),
            jax.ShapeDtypeStruct((8, DEVICES), F32),
            jax.ShapeDtypeStruct((TOKENS, 128), F32),
        ),
        in_specs=[SM, VM] + [ANY] * 4,
        out_specs=(VM,) * 4,
        scratch_shapes=[
            pltpu.VMEM((SPAN, 512), F32),
            pltpu.VMEM((64, ROWS[0]), BF16),
            pltpu.VMEM((64, ROWS[1]), BF16),
            pltpu.VMEM((ROWS[2], 128), BF16),
            pltpu.VMEM((ROWS[3], 256), BF16),
            pltpu.SemaphoreType.DMA((4,)),
        ],
        compiler_params=pltpu.CompilerParams(vmem_limit_bytes=VMEM_LIMIT),
        name="lookup",
    )(me, ids, *tables)


def moments(values):
    mean = jnp.mean(values, axis=-1, keepdims=True)
    centred = values - mean
    scale = lax.rsqrt(jnp.mean(centred * centred, axis=-1, keepdims=True) + 1e-05)
    return centred * scale, scale


def norm_back(grad, normed, scale):
    inner = jnp.mean(grad * normed, axis=-1, keepdims=True)
    return scale * (grad - jnp.mean(grad, axis=-1, keepdims=True) - normed * inner)


def sigmoid(values):
    return 0.5 * jnp.tanh(0.5 * values) + 0.5


def layer_kernel(
    got_ref, cols_ref, w_hbm, cot_hbm, out_hbm, first_ref, second_ref, g_hbm,
    rows_s, emb_s, norm_s, slope_s, act_s, att_s, gated_s, datt_s, dpre_s, demb_s, place_s,
    w_ref, cot_ref, out_ref, g_ref, in_sem, out_sem,
):
    half = 128
    pieces = (slice(0, 512), slice(512, 2560), slice(2560, 3072))
    loads = [
        pltpu.make_async_copy(w_hbm.at[:, part], w_ref.at[:, part], in_sem.at[i])
        for i, part in enumerate(pieces)
    ]
    loads.append(pltpu.make_async_copy(cot_hbm, cot_ref, in_sem.at[3]))
    for copy in loads:
        copy.start()
    stores = [
        pltpu.make_async_copy(g_ref.at[:, part], g_hbm.at[:, part], out_sem.at[i])
        for i, part in enumerate(pieces)
    ]
    stores.append(pltpu.make_async_copy(out_ref, out_hbm, out_sem.at[3]))
    loads[0].wait()
    proj = w_ref[:, 0:512]

    def begin(s, _):
        at = pl.ds(pl.multiple_of(s * SPAN, SPAN), SPAN)
        owner = cols_ref[at, 0:1].astype(I32)
        table = cols_ref[at, 1:2]
        rank = cols_ref[at, 3:4]
        hot = (owner == lax.broadcasted_iota(I32, (SPAN, DEVICES), 1)).astype(BF16)
        lane = lax.broadcasted_iota(I32, (SPAN, half), 1)
        kind = jnp.where(lane < 64, 0.0, 1.0)
        got = dot(hot, got_ref[0])
        first = rank == 0.0
        ab = jnp.where((table == kind), jnp.where(first, got[:, 0:128], got[:, 128:256]), 0.0)
        c = jnp.where(table == 2.0, jnp.where(first, got[:, 256:384], got[:, 384:512]), 0.0)
        got = dot(hot, got_ref[1])
        d = jnp.where(table == 3.0, jnp.where(first, got[:, 0:256], got[:, 256:512]), 0.0)
        rows = jnp.concatenate([ab, c, d], axis=1).astype(BF16)
        rows_s[at, :] = rows
        emb = dot(rows, proj).astype(BF16)
        emb_s[at, :] = emb
        normed, _scale = moments(emb.astype(F32))
        norm_s[at, :] = normed.astype(BF16)
        return 0

    lax.fori_loop(0, 2, begin, 0)

    loads[1].wait()

    def project(i, _):
        s, part = i // 4, lax.rem(i, 4)
        at = pl.ds(pl.multiple_of(s * SPAN, SPAN), SPAN)
        lanes = pl.ds(pl.multiple_of(part * 512, 512), 512)
        pre = dot(norm_s[at, :], w_ref[:, pl.ds(pl.multiple_of(part * 512 + 512, 512), 512)])
        sig = sigmoid(pre)
        act = pre * sig
        slope_s[at, lanes] = sig + act * (1.0 - sig)
        act_s[at, lanes] = act.astype(BF16)
        return 0

    lax.fori_loop(0, 8, project, 0)

    blocks = ((0, 256), (256, 384))

    def head_lanes(kind, head):
        return pl.ds(pl.multiple_of(kind * 512 + head * HEAD, HEAD), HEAD)

    def kept(low, high, length):
        row = lax.broadcasted_iota(I32, (high - low, high), 0) + low
        column = lax.broadcasted_iota(I32, (high - low, high), 1)
        return (column <= row) & (column.astype(F32) < length)

    def attend(i, _):
        s, head = i // 4, lax.rem(i, 4)
        at = pl.ds(pl.multiple_of(s * SPAN, SPAN), SPAN)
        length = cols_ref[at, 2:3]
        value = act_s[at, head_lanes(1, head)]
        query = act_s[at, head_lanes(2, head)]
        key = act_s[at, head_lanes(3, head)]
        results = []
        for low, high in blocks:
            scores = dot(query[low:high], key[:high], 1, 1) * HEAD**-0.5
            keep = kept(low, high, length[low:high])
            attn = jnp.where(keep, scores * sigmoid(scores), 0.0).astype(BF16)
            results.append(dot(attn, value[:high]))
        att_s[at, head_lanes(0, head)] = jnp.concatenate(results, axis=0)
        return 0

    lax.fori_loop(0, 8, attend, 0, unroll=UNROLL)
    loads[2].wait()
    loads[3].wait()
    out_w = w_ref[:, 2560:3072]

    def middle(s, _):
        at = pl.ds(pl.multiple_of(s * SPAN, SPAN), SPAN)
        normed, scale = moments(att_s[at, :])
        gate = act_s[at, 0:512].astype(F32)
        gated = (normed * gate).astype(BF16)
        gated_s[at, :] = gated
        branch = dot(gated, out_w)
        out_ref[at, :] = (emb_s[at, :].astype(F32) + branch).astype(BF16)
        where = lax.broadcasted_iota(I32, (SPAN, 1), 0).astype(F32)
        grad = jnp.where(where < cols_ref[at, 2:3], cot_ref[at, :], jnp.zeros((), BF16))
        demb_s[at, :] = grad
        d_gated = dot(grad, out_w, 1, 1).astype(BF16).astype(F32)
        d_gate = (d_gated * normed).astype(BF16).astype(F32)
        dpre_s[at, 0:512] = (d_gate * slope_s[at, 0:512]).astype(BF16)
        datt_s[at, :] = norm_back(d_gated * gate, normed, scale).astype(BF16)
        return 0

    lax.fori_loop(0, 2, middle, 0)
    stores[3].start()
    g_ref[:, 2560:3072] = dot(gated_s[...], demb_s[...], 0, 0).astype(BF16)
    stores[2].start()

    def attend_back(i, _):
        s, head = i // 4, lax.rem(i, 4)
        at = pl.ds(pl.multiple_of(s * SPAN, SPAN), SPAN)
        length = cols_ref[at, 2:3]
        value = act_s[at, head_lanes(1, head)]
        query = act_s[at, head_lanes(2, head)]
        key = act_s[at, head_lanes(3, head)]
        d_att = datt_s[at, head_lanes(0, head)]
        d_query, d_key, d_value = [], [], []
        for low, high in blocks:
            scores = dot(query[low:high], key[:high], 1, 1) * HEAD**-0.5
            sig = sigmoid(scores)
            act = scores * sig
            keep = kept(low, high, length[low:high])
            attn = jnp.where(keep, act, 0.0).astype(BF16)
            d_attn = dot(d_att[low:high], value[:high], 1, 1).astype(BF16).astype(F32)
            slope = sig + act * (1.0 - sig)
            d_scores = (jnp.where(keep, d_attn * slope, 0.0) * HEAD**-0.5).astype(BF16)
            d_value.append(dot(attn, d_att[low:high], 0, 0))
            d_query.append(dot(d_scores, key[:high]))
            d_key.append(dot(d_scores, query[low:high], 0, 0))

        def whole(parts):
            return jnp.concatenate([parts[0] + parts[1][:256], parts[1][256:]], axis=0)

        grads = (whole(d_value), jnp.concatenate(d_query, axis=0), whole(d_key))
        for kind, grad in enumerate(grads):
            lanes = head_lanes(kind + 1, head)
            rounded = grad.astype(BF16).astype(F32)
            dpre_s[at, lanes] = (rounded * slope_s[at, lanes]).astype(BF16)
        return 0

    lax.fori_loop(0, 8, attend_back, 0, unroll=UNROLL)

    def first_weight(part, _):
        lanes = pl.ds(pl.multiple_of(part * 512, 512), 512)
        wide = pl.ds(pl.multiple_of(part * 512 + 512, 512), 512)
        g_ref[:, wide] = dot(norm_s[...], dpre_s[:, lanes], 0, 0).astype(BF16)
        return 0

    lax.fori_loop(0, 4, first_weight, 0)
    stores[1].start()

    def finish(s, _):
        at = pl.ds(pl.multiple_of(s * SPAN, SPAN), SPAN)
        d_normed = dot(dpre_s[at, 0:512], w_ref[:, 512:1024], 1, 1)
        for part in range(1, 4):
            lanes = slice(part * 512, part * 512 + 512)
            wide = slice(part * 512 + 512, part * 512 + 1024)
            d_normed = d_normed + dot(dpre_s[at, lanes], w_ref[:, wide], 1, 1)
        normed, scale = moments(emb_s[at, :].astype(F32))
        back = norm_back(d_normed.astype(BF16).astype(F32), normed, scale)
        d_emb = (demb_s[at, :].astype(F32) + back).astype(BF16)
        demb_s[at, :] = d_emb
        d_rows = dot(d_emb, proj, 1, 1)
        table = cols_ref[at, 1:2]
        rank = cols_ref[at, 3:4]
        lane = lax.broadcasted_iota(I32, (SPAN, half), 1)
        kind = jnp.where(lane < 64, 0.0, 1.0)
        for k in range(2):
            match = rank == float(k)
            low = k * 128
            place_s[at, low : low + 128] = jnp.where(
                (table == kind) & match, d_rows[:, 0:128], 0.0
            ).astype(BF16)
            place_s[at, 256 + low : 384 + low] = jnp.where(
                (table == 2.0) & match, d_rows[:, 128:256], 0.0
            ).astype(BF16)
            low = 512 + k * 256
            place_s[at, low : low + 256] = jnp.where(
                (table == 3.0) & match, d_rows[:, 256:512], 0.0
            ).astype(BF16)
        return 0

    lax.fori_loop(0, 2, finish, 0)
    g_ref[:, 0:512] = dot(rows_s[...], demb_s[...], 0, 0).astype(BF16)
    stores[0].start()
    owner = cols_ref[:, 0:1].astype(I32)
    hot = (owner == lax.broadcasted_iota(I32, (TOKENS, DEVICES), 1)).astype(BF16)
    first_ref[...] = dot(hot, place_s[:, 0:512], 0, 0).astype(BF16)
    second_ref[...] = dot(hot, place_s[:, 512:1024], 0, 0).astype(BF16)
    for copy in stores:
        copy.wait()


def layer(got, cols, weights, cotangent):
    def vmem(width, kind=BF16):
        return pltpu.VMEM((TOKENS, width), kind)

    return pl.pallas_call(
        layer_kernel,
        out_shape=(
            jax.ShapeDtypeStruct((TOKENS, WIDTH), BF16),
            jax.ShapeDtypeStruct((DEVICES, 512), BF16),
            jax.ShapeDtypeStruct((DEVICES, 512), BF16),
            jax.ShapeDtypeStruct((512, 3072), BF16),
        ),
        in_specs=[VM, VM, ANY, ANY],
        out_specs=(ANY, VM, VM, ANY),
        scratch_shapes=[
            vmem(512), vmem(512), vmem(512), vmem(2048, F32), vmem(2048), vmem(512, F32),
            vmem(512), vmem(512), vmem(2048), vmem(512), vmem(1024),
            pltpu.VMEM((512, 3072), BF16), vmem(512), vmem(512), pltpu.VMEM((512, 3072), BF16),
            pltpu.SemaphoreType.DMA((4,)), pltpu.SemaphoreType.DMA((4,)),
        ],
        compiler_params=pltpu.CompilerParams(vmem_limit_bytes=VMEM_LIMIT),
        name="layer",
    )(got, cols, weights, cotangent)


def scatter_kernel(
    got_ref, wanted_ref, total_ref, a_hbm, b_hbm, c_hbm, d_hbm, proj_ref, in_ref, out_ref,
    a_ref, b_ref, c_ref, d_ref, sem,
):
    stores = []
    proj_ref[...] = total_ref[:, 0:512].astype(F32)
    in_ref[...] = total_ref[:, 512:2560].astype(F32)
    out_ref[...] = total_ref[:, 2560:3072].astype(F32)
    row_form = wanted_ref[...]
    padded = jnp.concatenate([row_form, jnp.zeros((120, DEVICES), F32)], axis=0)
    col_form = jnp.transpose(padded)
    pairs = ((a_ref, a_hbm), (b_ref, b_hbm), (c_ref, c_hbm), (d_ref, d_hbm))
    for which, (grad_ref, grad_hbm) in enumerate(pairs):
        fold, rows = FOLD[which], ROWS[which]
        deep = rows // fold
        width = 256 // fold
        spread, inners = [], []
        for rank in range(2):
            row = col_form[:, rank * 4 + which : rank * 4 + which + 1].astype(I32)
            block = row // deep
            at = (0, 64, 256, 0)[which] + rank * (128, 128, 128, 256)[which]
            value = got_ref[which // 3, :, at : at + width].astype(F32)
            spread.append(
                jnp.concatenate([jnp.where(block == q, value, 0.0) for q in range(fold)], axis=1)
            )
            if which < 2:
                inners.append(row - block * deep)
            else:
                line = row_form[rank * 4 + which : rank * 4 + which + 1].astype(I32)
                inners.append(line - (line // deep) * deep)
        values = jnp.concatenate(spread, axis=0).astype(BF16)
        if which < 2:
            inner = jnp.concatenate(inners, axis=0)
            flipped = jnp.transpose(values.astype(F32)).astype(BF16)
            for at in range(0, deep, 512):
                hot = (inner == lax.broadcasted_iota(I32, (512, 512), 1) + at).astype(BF16)
                summed = dot(flipped, hot).astype(BF16)
                for q in range(fold):
                    grad_ref[:, q * deep + at : q * deep + at + 512] = summed[
                        q * width : (q + 1) * width
                    ]
        else:
            inner = jnp.concatenate(inners, axis=1)
            for at in range(0, deep, 512):
                hot = (inner == lax.broadcasted_iota(I32, (512, 512), 0) + at).astype(BF16)
                summed = dot(hot, values).astype(BF16)
                for q in range(fold):
                    grad_ref[q * deep + at : q * deep + at + 512, :] = summed[
                        :, q * width : (q + 1) * width
                    ]
        copy = pltpu.make_async_copy(grad_ref, grad_hbm, sem.at[which])
        copy.start()
        stores.append(copy)
    for copy in stores:
        copy.wait()


def scatter(got, wanted, totals):
    return pl.pallas_call(
        scatter_kernel,
        out_shape=(
            jax.ShapeDtypeStruct((64, ROWS[0]), BF16),
            jax.ShapeDtypeStruct((64, ROWS[1]), BF16),
            jax.ShapeDtypeStruct((ROWS[2], 128), BF16),
            jax.ShapeDtypeStruct((ROWS[3], 256), BF16),
            jax.ShapeDtypeStruct((16, 512), F32),
            jax.ShapeDtypeStruct((16, 2048), F32),
            jax.ShapeDtypeStruct((16, 512), F32),
        ),
        in_specs=[VM, VM, VM],
        out_specs=(ANY,) * 4 + (VM,) * 3,
        scratch_shapes=[
            pltpu.VMEM((64, ROWS[0]), BF16),
            pltpu.VMEM((64, ROWS[1]), BF16),
            pltpu.VMEM((ROWS[2], 128), BF16),
            pltpu.VMEM((ROWS[3], 256), BF16),
            pltpu.SemaphoreType.DMA((4,)),
        ],
        compiler_params=pltpu.CompilerParams(vmem_limit_bytes=VMEM_LIMIT),
        name="scatter",
    )(got, wanted, totals)


def add(*values):
    total = values[0].astype(F32)
    for value in values[1:]:
        total = total + value.astype(F32)
    return total


def deliver_kernel(
    first_ref, second_ref, g_ref, rows_ref, total_ref,
    across, pair, one, two, line, three, four, parts, column, mine, whole, *scratch,
):
    dp, xy, core, z = place()
    (x, right, left, to_right, to_left), (y, up, down, to_up, to_down) = near()
    far_x, far_y = lax.rem(x + 2, NX), lax.rem(y + 2, NY)
    link = Sender(*scratch[-2:])
    swap = Swap(link, first_ref, second_ref, rows_ref, *scratch[:-2])
    greet(swap.along_z + swap.along_dp)
    partner = peers()[2][0]
    start = link.start

    def meet(px, py, part):
        there = (px, py, 1 - core, part)
        return start(g_ref.at[there], across.at[px, py, part], partner)

    def join(px, py, part):
        for k in range(4):
            qx, qy = (px, k) if py is EVERY else (k, py)
            pair[qx, qy, part] = add(g_ref[qx, qy, core, part], across[qx, qy, part]).astype(BF16)

    far = [meet(far_x, EVERY, 0), meet(EVERY, far_y, 1)]
    high = swap.begin_high()
    sides = [
        meet(right, EVERY, 0), meet(left, EVERY, 0), meet(EVERY, up, 1), meet(EVERY, down, 1)
    ]
    centre = [meet(x, EVERY, 0), meet(EVERY, y, 1)]
    finish(far)
    join(far_x, EVERY, 0)
    join(EVERY, far_y, 1)
    steps = [
        start(pair.at[far_x, LOW, 0], one.at[0], to_right),
        start(pair.at[far_x, HIGH, 0], one.at[1], to_left),
        start(pair.at[LOW, far_y, 1], one.at[2], to_up),
        start(pair.at[HIGH, far_y, 1], one.at[3], to_down),
    ]
    low = swap.begin_low()
    finish(sides)
    join(right, EVERY, 0)
    join(left, EVERY, 0)
    join(EVERY, up, 1)
    join(EVERY, down, 1)
    finish(steps)
    for k in range(2):
        pair[right, k, 0] = add(pair[right, k, 0], one[0, k]).astype(BF16)
        pair[left, 2 + k, 0] = add(pair[left, 2 + k, 0], one[1, k]).astype(BF16)
        pair[k, up, 1] = add(pair[k, up, 1], one[2, k]).astype(BF16)
        pair[2 + k, down, 1] = add(pair[2 + k, down, 1], one[3, k]).astype(BF16)
    steps = [
        start(pair.at[right, :, 0], two.at[0], to_right),
        start(pair.at[left, :, 0], two.at[1], to_left),
        start(pair.at[:, up, 1], two.at[2], to_up),
        start(pair.at[:, down, 1], two.at[3], to_down),
    ]
    finish(low)
    low = swap.turn_low()
    finish(centre)
    join(x, EVERY, 0)
    join(EVERY, y, 1)
    finish(steps)
    for k in range(4):
        line[0, k] = add(pair[x, k, 0], two[0, k], two[1, k]).astype(BF16)
        line[1, k] = add(pair[k, y, 1], two[2, k], two[3, k]).astype(BF16)
    steps = [
        start(line.at[0, far_y, :, AHEAD], three.at[0], to_up),
        start(line.at[0, far_y, :, BEHIND], three.at[1], to_down),
        start(line.at[1, far_x, :, AHEAD], three.at[2], to_right),
        start(line.at[1, far_x, :, BEHIND], three.at[3], to_left),
    ]
    finish(high)
    high = swap.turn_high()
    finish(steps)
    line[0, up, :, AHEAD] = add(line[0, up, :, AHEAD], three[0]).astype(BF16)
    line[0, down, :, BEHIND] = add(line[0, down, :, BEHIND], three[1]).astype(BF16)
    line[1, right, :, AHEAD] = add(line[1, right, :, AHEAD], three[2]).astype(BF16)
    line[1, left, :, BEHIND] = add(line[1, left, :, BEHIND], three[3]).astype(BF16)
    finish(
        [
            start(line.at[0, up], four.at[0], to_up),
            start(line.at[0, down], four.at[1], to_down),
            start(line.at[1, right], four.at[2], to_right),
            start(line.at[1, left], four.at[3], to_left),
        ]
    )
    for q in range(NZ):
        lanes = pl.ds(q * 384, 384)
        parts[q, 0] = add(line[0, y, :, lanes], four[0, :, lanes], four[1, :, lanes]).astype(BF16)
        parts[q, 1] = add(line[1, x, :, lanes], four[2, :, lanes], four[3, :, lanes]).astype(BF16)
    steps = [start(parts.at[t[1]], column.at[i], t) for i, t in enumerate(swap.along_z)]
    finish(low)
    swap.end_low()
    finish(steps)
    mine[...] = add(parts[z], *[column[k] for k in range(NZ - 1)]).astype(BF16)
    steps = [start(mine, whole.at[z], t) for t in swap.along_z]
    whole[pl.ds(z, 1)] = mine[...][None]
    finish(high + steps)
    for half in range(2):
        for q in range(NZ):
            total_ref[half * 8 : half * 8 + 8, q * 384 : q * 384 + 384] = whole[q, half]


def deliver(first, second, terms):
    return pl.pallas_call(
        deliver_kernel,
        out_shape=(
            jax.ShapeDtypeStruct((2, 32, 8, 512), BF16),
            jax.ShapeDtypeStruct((16, 3072), BF16),
        ),
        in_specs=[VM] * 3,
        out_specs=(VM, VM),
        scratch_shapes=[
            pltpu.VMEM((4, 4, 2, 8, 3072), BF16),
            pltpu.VMEM((4, 4, 2, 8, 3072), BF16),
            pltpu.VMEM((4, 2, 8, 3072), BF16),
            pltpu.VMEM((4, 4, 8, 3072), BF16),
            pltpu.VMEM((2, 4, 8, 3072), BF16),
            pltpu.VMEM((4, 8, 1536), BF16),
            pltpu.VMEM((4, 8, 3072), BF16),
            pltpu.VMEM((8, 2, 8, 384), BF16),
            pltpu.VMEM((7, 2, 8, 384), BF16),
            pltpu.VMEM((2, 8, 384), BF16),
            pltpu.VMEM((8, 2, 8, 384), BF16),
        ]
        + SWAP_SHAPES
        + sems(114),
        compiler_params=comm_params(3),
        name="deliver",
    )(first, second, terms)


def shards(
    item_ids, table_ids, lengths, assignment,
    table_a, table_b, table_c, table_d,
    proj_weight, in_weight, out_weight, cotangent,
):
    ids, full = share(
        item_ids, table_ids, lengths, assignment, (proj_weight, in_weight, out_weight)
    )
    me = (lax.axis_index("dp") * NZ + lax.axis_index("table")).astype(I32).reshape(1)
    first, second, wanted, cols = lookup(
        me, ids.reshape(DEVICES, 8, 128), (table_a.T, table_b.T, table_c, table_d)
    )
    got = fetch(first, second.reshape(32, 8, 512))
    output, first, second, terms = layer(
        got.reshape(2, DEVICES, 512),
        cols,
        full.reshape(512, 3072),
        cotangent.reshape(TOKENS, WIDTH),
    )
    arrived, totals = deliver(
        first, second.reshape(32, 8, 512), terms.reshape(NX, NY, 2, 2, 8, 3072)
    )
    grads = scatter(arrived.reshape(2, DEVICES, 512), wanted, totals)
    return (
        output.reshape(2, SPAN, WIDTH),
        grads[0].T,
        grads[1].T,
        *grads[2:],
    )


def solution(mesh):
    both = ("dp", "table")
    return jax.shard_map(
        shards,
        mesh=mesh,
        in_specs=(
            P(both, None), P(both, None), P(both), P(both),
            P(both, None), P(both, None), P(both, None), P(both, None),
            P("dp", None), P("dp", None), P("dp", None), P(both, None, None),
        ),
        out_specs=(
            P(both, None, None),
            P(both, None), P(both, None), P(both, None), P(both, None),
            P("dp", None), P("dp", None), P("dp", None),
        ),
        check_vma=False,
    )
```

```python
import functools

import jax
import jax.numpy as jnp
from jax import lax
from jax.experimental import pallas as pl
from jax.experimental.pallas import tpu as pltpu
from jax.sharding import PartitionSpec as P

MESH = pl.DeviceIdType.MESH
VM = pl.BlockSpec(memory_space=pltpu.VMEM)
F32, BF16, I32 = jnp.float32, jnp.bfloat16, jnp.int32
NX, NY, NZ, PLANE = 4, 4, 8, 16
DEVICES = 256
HEADS, HEAD = 4, 128
SPAN, TOKENS, WIDTH = 384, 768, 512
ROWS = (12288, 12288, 6144, 2048)
FOLD = (4, 4, 2, 1)
TABLE_BITS = 22
KEY = 1024
NONE = 16383.0 * KEY
VMEM_LIMIT = 60 << 20
UNROLL = 4
ANY = pl.BlockSpec(memory_space=pl.ANY)


def place():
    dp, z = lax.axis_index("dp"), lax.axis_index("table")
    return dp, dp // 2, lax.rem(dp, 2), z


def plane_peer(xy, k):
    x = lax.rem(xy // NY + k // NY, NX)
    y = lax.rem(lax.rem(xy, NY) + k % NY, NY)
    return x * NY + y


def peers():
    dp, xy, core, z = place()
    along_z = [(dp, lax.rem(z + k, NZ)) for k in range(1, NZ)]
    in_plane = [(plane_peer(xy, k) * 2 + core, z) for k in range(1, PLANE)]
    return along_z, in_plane, [(xy * 2 + (1 - core), z)]


def near():
    dp, xy, core, z = place()
    x, y = xy // NY, lax.rem(xy, NY)
    right, left = lax.rem(x + 1, NX), lax.rem(x + NX - 1, NX)
    up, down = lax.rem(y + 1, NY), lax.rem(y + NY - 1, NY)

    def at(px, py):
        return ((px * NY + py) * 2 + core, z)

    return (x, right, left, at(right, y), at(left, y)), (y, up, down, at(x, up), at(x, down))


def greet(targets):
    barrier = pltpu.get_barrier_semaphore()
    for dp, z in targets:
        pl.semaphore_signal(barrier, inc=1, device_id=(dp, z), device_id_type=MESH)
    pl.semaphore_wait(barrier, len(targets))


def send(src, dst, send_sem, recv_sem, target):
    copy = pltpu.make_async_remote_copy(
        src_ref=src,
        dst_ref=dst,
        send_sem=send_sem,
        recv_sem=recv_sem,
        device_id=target,
        device_id_type=MESH,
    )
    copy.start()
    return copy


def dot(a, b, da=1, db=0):
    return lax.dot_general(a, b, (((da,), (db,)), ((), ())), preferred_element_type=F32)


class Sender:
    def __init__(self, send_sem, recv_sem):
        self.sems, self.used = (send_sem, recv_sem), 0

    def start(self, src, dst, target):
        at, self.used = self.used, self.used + 1
        return send(src, dst, self.sems[0].at[at], self.sems[1].at[at], target)

    def move(self, ref, target):
        return self.start(ref, ref, target)


def finish(copies):
    for copy in copies:
        copy.wait()


EVERY, LOW, HIGH = slice(None), pl.ds(0, 2), pl.ds(2, 2)
AHEAD, BEHIND = pl.ds(0, 1536), pl.ds(1536, 1536)


def sems(count):
    return [pltpu.SemaphoreType.DMA((count,)), pltpu.SemaphoreType.DMA((count,))]


def comm_params(collective):
    return pltpu.CompilerParams(
        collective_id=collective, has_side_effects=True, vmem_limit_bytes=VMEM_LIMIT
    )


SM = pl.BlockSpec(memory_space=pltpu.SMEM)


class Swap:
    def __init__(self, link, first_ref, second_ref, out_ref, by_z, from_z, by_dp, from_dp, again_z, from_z2):
        self.link, self.first, self.second, self.out = link, first_ref, second_ref, out_ref
        self.by_z, self.from_z, self.by_dp = by_z, from_z, by_dp
        self.from_dp, self.again_z, self.from_z2 = from_dp, again_z, from_z2
        self.dp, xy, core, self.z = place()
        self.along_z, in_plane, partner = peers()
        others = [(plane_peer(xy, k) * 2 + (1 - core), self.z) for k in range(1, PLANE)]
        self.along_dp = in_plane + partner + others
        i = lax.broadcasted_iota(I32, (DEVICES, DEVICES), 0)
        j = lax.broadcasted_iota(I32, (DEVICES, DEVICES), 1)
        self.z_first = (j == (i & 31) * 8 + (i >> 5)).astype(BF16)
        self.dp_first = (j == (i & 7) * 32 + (i >> 3)).astype(BF16)

    def ready_high(self):
        self.by_z[...] = self.arrange(self.z_first, self.first, (NZ, 32, 512))
        self.from_z[pl.ds(self.z, 1)] = self.by_z[pl.ds(self.z, 1)]

    def ready_low(self):
        self.from_dp[pl.ds(self.dp, 1)] = self.second[pl.ds(self.dp, 1)]

    def arrange(self, matrix, ref, dims):
        return dot(matrix, ref[...].reshape(DEVICES, 512)).astype(BF16).reshape(dims)

    def begin_high(self):
        return [self.link.start(self.by_z.at[t[1]], self.from_z.at[self.z], t) for t in self.along_z]

    def begin_low(self):
        return [
            self.link.start(self.second.at[t[0]], self.from_dp.at[self.dp], t)
            for t in self.along_dp
        ]

    def turn_low(self):
        self.again_z[...] = self.arrange(self.z_first, self.from_dp, (NZ, 32, 512))
        self.from_z2[pl.ds(self.z, 1)] = self.again_z[pl.ds(self.z, 1)]
        return [
            self.link.start(self.again_z.at[t[1]], self.from_z2.at[self.z], t)
            for t in self.along_z
        ]

    def turn_high(self):
        self.by_dp[...] = self.arrange(self.dp_first, self.from_z, (32, NZ, 512))
        self.out[0, pl.ds(self.dp, 1)] = self.by_dp[pl.ds(self.dp, 1)]
        return [
            self.link.start(self.by_dp.at[t[0]], self.out.at[0, self.dp], t) for t in self.along_dp
        ]

    def end_low(self):
        self.out[1] = self.arrange(self.dp_first, self.from_z2, (32, NZ, 512))


SWAP_SHAPES = [
    pltpu.VMEM((8, 32, 512), BF16),
    pltpu.VMEM((8, 32, 512), BF16),
    pltpu.VMEM((32, 8, 512), BF16),
    pltpu.VMEM((32, 8, 512), BF16),
    pltpu.VMEM((8, 32, 512), BF16),
    pltpu.VMEM((8, 32, 512), BF16),
]


def smallest_two(keys):
    first = jnp.full((8, keys.shape[1]), NONE, F32)
    second = first
    for at in range(0, keys.shape[0], 8):
        value = keys[at : at + 8]
        second = jnp.minimum(second, jnp.maximum(first, value))
        first = jnp.minimum(first, value)
    low = jnp.min(first, axis=0, keepdims=True)
    high = jnp.min(jnp.where(first == low, second, first), axis=0, keepdims=True)
    return low, high


def front_kernel(
    items_ref, tables_ref, lengths_ref, targets_ref, proj_ref, in_ref, wout_ref,
    a_hbm, b_hbm, c_hbm, d_hbm,
    out_ref, full_ref, wanted_ref, cols_ref,
    ids_ref, moved, first_ref, second_ref, a_ref, b_ref, c_ref, d_ref, sem, *scratch,
):
    *buffers, send_sem, recv_sem = scratch
    hbm, tables = (a_hbm, b_hbm, c_hbm, d_hbm), (a_ref, b_ref, c_ref, d_ref)
    loads = [pltpu.make_async_copy(hbm[i], tables[i], sem.at[i]) for i in range(4)]
    for copy in loads:
        copy.start()
    dp, xy, core, z = place()
    me = dp * NZ + z
    (x, right, left, to_right, to_left), (y, up, down, to_up, to_down) = near()
    far_x, far_y = lax.rem(x + 2, NX), lax.rem(y + 2, NY)
    to_far_x, to_far_y = ((far_x * NY + y) * 2 + core, z), ((x * NY + far_y) * 2 + core, z)
    lane = lax.broadcasted_iota(I32, (1, 128), 1)
    events = tables_ref[...] * (1 << TABLE_BITS) + items_ref[...]
    lines = []
    for s in range(2):
        lines += [events[s : s + 1, r * 128 : r * 128 + 128] for r in range(3)]
        lines.append(jnp.where(lane == 0, lengths_ref[s], jnp.where(lane == 1, targets_ref[s], 0)))
    ids_ref[x, y, core, z] = jnp.concatenate(lines, axis=0)
    for half in range(2):
        rows = slice(half * 8, half * 8 + 8)
        full_ref[x, y, core, half, :, 0:512] = proj_ref[rows, :]
        full_ref[x, y, core, half, :, 512:2560] = in_ref[rows, :]
        full_ref[x, y, core, half, :, 2560:3072] = wout_ref[rows, :]
    along_z, _plane, partner = peers()
    partner = partner[0]
    near_x, near_y = [to_right, to_left], [to_up, to_down]
    link = Sender(send_sem, recv_sem)
    swap = Swap(link, first_ref, second_ref, out_ref, *buffers)
    greet(swap.along_z + swap.along_dp)

    def ids(px, py, low):
        return ids_ref.at[px, py, core, pl.ds(low, 4)]

    def w(px, py, part):
        return full_ref.at[px, py, core, part]

    own = ids_ref.at[x, y, core, z]
    one = [link.move(own, t) for t in along_z]
    w_one = [link.move(w(x, y, 0), t) for t in near_y] + [link.move(w(x, y, 1), t) for t in near_x]
    finish(one)
    two = [link.move(ids(x, y, 0), t) for t in near_y + [to_far_y]]
    two += [link.move(ids(x, y, 4), t) for t in near_x + [to_far_x]]
    finish(w_one)
    w_two = [
        link.move(full_ref.at[x, down, core, 0, :, AHEAD], to_up),
        link.move(full_ref.at[x, up, core, 0, :, BEHIND], to_down),
        link.move(full_ref.at[left, y, core, 1, :, AHEAD], to_right),
        link.move(full_ref.at[right, y, core, 1, :, BEHIND], to_left),
    ]
    finish(two)
    three = [link.move(ids(x, EVERY, 0), t) for t in [to_far_x] + near_x]
    three += [link.move(ids(EVERY, y, 4), t) for t in [to_far_y] + near_y]
    across = [link.move(ids(x, EVERY, 0), partner), link.move(ids(EVERY, y, 4), partner)]
    finish(w_two)
    w_three = [
        link.move(w(x, EVERY, 0), to_right),
        link.move(w(x, EVERY, 0), to_left),
        link.move(w(EVERY, y, 1), to_up),
        link.move(w(EVERY, y, 1), to_down),
    ]
    w_across = [link.move(w(x, EVERY, 0), partner), link.move(w(EVERY, y, 1), partner)]
    finish(three)
    across += [link.move(ids(side, EVERY, 0), partner) for side in (right, left, far_x)]
    across += [link.move(ids(EVERY, side, 4), partner) for side in (up, down, far_y)]
    finish(across)

    def line_of(j):
        return ids_ref[:, :, :, :, j, :].reshape(DEVICES, 128)

    words = jnp.concatenate(
        [
            jnp.concatenate([line_of(4 * s + r) for r in range(3)], axis=1)
            for s in range(2)
        ],
        axis=0,
    )
    extra = jnp.concatenate([line_of(3), line_of(7)], axis=0)
    lengths = extra[:, 0:1].astype(F32)
    targets = extra[:, 1:2]
    arranged = (targets & 1) * DEVICES + (targets >> 1)
    slots = lax.broadcasted_iota(I32, (512, 512), 1)
    goes = (arranged == slots).astype(BF16)
    total = None
    for shift in (16, 8, 0):
        part = ((words >> shift) & 255).astype(F32).astype(BF16)
        piece = dot(part, goes, 0, 0)
        total = piece if total is None else total * 256.0 + piece
    moved[...] = total

    place_of = lax.broadcasted_iota(I32, (SPAN, 512), 0).astype(F32)
    lows, highs = [], []
    for which in range(4):
        start = which * (1 << TABLE_BITS) + me * ROWS[which]
        local = moved[...] - start.astype(F32)
        held = (local >= 0.0) & (local < float(ROWS[which]))
        keys = jnp.where(held, local * float(KEY) + place_of, NONE)
        low, high = smallest_two(keys)
        low_a, high_a = low[:, :DEVICES], high[:, :DEVICES]
        low_b, high_b = low[:, DEVICES:] + float(SPAN), high[:, DEVICES:] + float(SPAN)
        lows.append(jnp.minimum(low_a, low_b))
        highs.append(jnp.minimum(jnp.maximum(low_a, low_b), jnp.minimum(high_a, high_b)))
    row_form = jnp.floor(jnp.concatenate(lows + highs, axis=0) * (1.0 / KEY))
    wanted_ref[...] = row_form
    padded = jnp.concatenate([row_form, jnp.zeros((120, DEVICES), F32)], axis=0)
    col_form = jnp.transpose(padded)

    def find(which):
        table_ref = tables[which]
        loads[which].wait()
        fold, rows = FOLD[which], ROWS[which]
        deep = rows // fold
        width = 256 // fold
        for rank in range(2):
            row = col_form[:, rank * 4 + which : rank * 4 + which + 1].astype(I32)
            block = row // deep
            inner = row - block * deep
            acc = jnp.zeros((DEVICES, 256), F32)
            tile = 1024
            for at in range(0, deep, tile):
                index = lax.broadcasted_iota(I32, (DEVICES, tile), 1) + at
                hot = (inner == index).astype(BF16)
                if which < 2:
                    piece = jnp.concatenate(
                        [table_ref[:, q * deep + at : q * deep + at + tile] for q in range(fold)],
                        axis=0,
                    )
                    acc = acc + dot(hot, piece, 1, 1)
                else:
                    piece = jnp.concatenate(
                        [table_ref[q * deep + at : q * deep + at + tile, :] for q in range(fold)],
                        axis=1,
                    )
                    acc = acc + dot(hot, piece)
            value = jnp.zeros((DEVICES, width), F32)
            for q in range(fold):
                value = value + jnp.where(block == q, acc[:, q * width : (q + 1) * width], 0.0)
            at = (0, 64, 256, 0)[which] + rank * (128, 128, 128, 256)[which]
            if which == 3:
                second_ref[:, :, at : at + width] = value.astype(BF16).reshape(32, NZ, width)
            else:
                first_ref[:, at : at + width] = value.astype(BF16)

    find(3)
    swap.ready_low()
    low = swap.begin_low()
    finish(w_three)
    w_four = [
        link.move(w(left, LOW, 0), to_right),
        link.move(w(right, HIGH, 0), to_left),
        link.move(w(LOW, down, 1), to_up),
        link.move(w(HIGH, up, 1), to_down),
    ]
    w_across += [link.move(w(side, EVERY, 0), partner) for side in (right, left)]
    w_across += [link.move(w(EVERY, side, 1), partner) for side in (up, down)]
    for which in range(3):
        find(which)
    swap.ready_high()
    high = swap.begin_high()
    finish(low)
    low = swap.turn_low()
    finish(w_four)
    w_across += [link.move(w(far_x, EVERY, 0), partner), link.move(w(EVERY, far_y, 1), partner)]

    pieces, spans = [], []
    for s in range(2):
        hit = targets == 2 * me + s
        pieces.append(jnp.sum(jnp.where(hit, words, 0), axis=0, keepdims=True))
        length = jnp.sum(jnp.where(hit, lengths, 0.0), axis=0, keepdims=True)
        spans.append(jnp.broadcast_to(length, (1, SPAN)))
    event = jnp.concatenate(pieces, axis=1)
    span = jnp.concatenate(spans, axis=1)
    table = event >> TABLE_BITS
    item = event & ((1 << TABLE_BITS) - 1)
    unit = jnp.where(table == 3, item >> 11, jnp.where(table == 2, item >> 11, item >> 12))
    third = jnp.floor((unit.astype(F32) + 0.5) * (1.0 / 3.0)).astype(I32)
    owner = jnp.where(table == 3, unit, third)
    per = jnp.where(table == 3, ROWS[3], jnp.where(table == 2, ROWS[2], ROWS[0]))
    local = item - owner * per
    order = lax.broadcasted_iota(I32, (1, TOKENS), 1)
    key = (local * KEY + order).astype(F32)
    bucket = (table * DEVICES + owner).astype(F32)
    lines = [owner.astype(F32), table.astype(F32), span, key, bucket]
    stacked = jnp.concatenate(lines + [jnp.zeros((123, TOKENS), F32)], axis=0)
    cols = jnp.transpose(stacked)
    ahead = (cols[:, 4:5] == bucket) & (key < cols[:, 3:4])
    rank = jnp.sum(jnp.where(ahead, 1.0, 0.0), axis=1, keepdims=True)
    lane = lax.broadcasted_iota(I32, (TOKENS, 128), 1)
    cols_ref[...] = jnp.where(lane == 3, rank, cols)

    finish(high)
    high = swap.turn_high()
    finish(low)
    swap.end_low()
    finish(high + w_across)


def front(items, tables, lengths, targets, weights, held):
    return pl.pallas_call(
        front_kernel,
        out_shape=(
            jax.ShapeDtypeStruct((2, 32, 8, 512), BF16),
            jax.ShapeDtypeStruct((NX, NY, 2, 2, 8, 3072), BF16),
            jax.ShapeDtypeStruct((8, DEVICES), F32),
            jax.ShapeDtypeStruct((TOKENS, 128), F32),
        ),
        in_specs=[VM, VM, SM, SM, VM, VM, VM] + [ANY] * 4,
        out_specs=(VM,) * 4,
        scratch_shapes=[
            pltpu.VMEM((NX, NY, 2, NZ, 8, 128), I32),
            pltpu.VMEM((SPAN, 512), F32),
            pltpu.VMEM((DEVICES, 512), BF16),
            pltpu.VMEM((32, NZ, 512), BF16),
            pltpu.VMEM((64, ROWS[0]), BF16),
            pltpu.VMEM((64, ROWS[1]), BF16),
            pltpu.VMEM((ROWS[2], 128), BF16),
            pltpu.VMEM((ROWS[3], 256), BF16),
            pltpu.SemaphoreType.DMA((4,)),
        ]
        + SWAP_SHAPES
        + sems(127),
        compiler_params=comm_params(1),
        name="front",
    )(items, tables, lengths, targets, *weights, *held)


def moments(values):
    mean = jnp.mean(values, axis=-1, keepdims=True)
    centred = values - mean
    scale = lax.rsqrt(jnp.mean(centred * centred, axis=-1, keepdims=True) + 1e-05)
    return centred * scale, scale


def norm_back(grad, normed, scale):
    inner = jnp.mean(grad * normed, axis=-1, keepdims=True)
    return scale * (grad - jnp.mean(grad, axis=-1, keepdims=True) - normed * inner)


def sigmoid(values):
    return 0.5 * jnp.tanh(0.5 * values) + 0.5


def layer_kernel(
    got_ref, cols_ref, w_hbm, cot_hbm, out_hbm, first_ref, second_ref, g_hbm,
    rows_s, emb_s, norm_s, slope_s, act_s, att_s, gated_s, datt_s, dpre_s, demb_s, place_s,
    w_ref, cot_ref, out_ref, g_ref, in_sem, out_sem,
):
    half = 128
    pieces = (slice(0, 512), slice(512, 2560), slice(2560, 3072))
    loads = [
        pltpu.make_async_copy(w_hbm.at[:, part], w_ref.at[:, part], in_sem.at[i])
        for i, part in enumerate(pieces)
    ]
    loads.append(pltpu.make_async_copy(cot_hbm, cot_ref, in_sem.at[3]))
    for copy in loads:
        copy.start()
    stores = [
        pltpu.make_async_copy(g_ref.at[:, part], g_hbm.at[:, part], out_sem.at[i])
        for i, part in enumerate(pieces)
    ]
    stores.append(pltpu.make_async_copy(out_ref, out_hbm, out_sem.at[3]))
    loads[0].wait()
    proj = w_ref[:, 0:512]

    def begin(s, _):
        at = pl.ds(pl.multiple_of(s * SPAN, SPAN), SPAN)
        owner = cols_ref[at, 0:1].astype(I32)
        table = cols_ref[at, 1:2]
        rank = cols_ref[at, 3:4]
        hot = (owner == lax.broadcasted_iota(I32, (SPAN, DEVICES), 1)).astype(BF16)
        lane = lax.broadcasted_iota(I32, (SPAN, half), 1)
        kind = jnp.where(lane < 64, 0.0, 1.0)
        got = dot(hot, got_ref[0])
        first = rank == 0.0
        ab = jnp.where((table == kind), jnp.where(first, got[:, 0:128], got[:, 128:256]), 0.0)
        c = jnp.where(table == 2.0, jnp.where(first, got[:, 256:384], got[:, 384:512]), 0.0)
        got = dot(hot, got_ref[1])
        d = jnp.where(table == 3.0, jnp.where(first, got[:, 0:256], got[:, 256:512]), 0.0)
        rows = jnp.concatenate([ab, c, d], axis=1).astype(BF16)
        rows_s[at, :] = rows
        emb = dot(rows, proj).astype(BF16)
        emb_s[at, :] = emb
        normed, _scale = moments(emb.astype(F32))
        norm_s[at, :] = normed.astype(BF16)
        return 0

    lax.fori_loop(0, 2, begin, 0)

    loads[1].wait()

    def project(i, _):
        s, part = i // 4, lax.rem(i, 4)
        at = pl.ds(pl.multiple_of(s * SPAN, SPAN), SPAN)
        lanes = pl.ds(pl.multiple_of(part * 512, 512), 512)
        pre = dot(norm_s[at, :], w_ref[:, pl.ds(pl.multiple_of(part * 512 + 512, 512), 512)])
        sig = sigmoid(pre)
        act = pre * sig
        slope_s[at, lanes] = sig + act * (1.0 - sig)
        act_s[at, lanes] = act.astype(BF16)
        return 0

    lax.fori_loop(0, 8, project, 0)

    blocks = ((0, 256), (256, 384))

    def head_lanes(kind, head):
        return pl.ds(pl.multiple_of(kind * 512 + head * HEAD, HEAD), HEAD)

    def kept(low, high, length):
        row = lax.broadcasted_iota(I32, (high - low, high), 0) + low
        column = lax.broadcasted_iota(I32, (high - low, high), 1)
        return (column <= row) & (column.astype(F32) < length)

    def attend(i, _):
        s, head = i // 4, lax.rem(i, 4)
        at = pl.ds(pl.multiple_of(s * SPAN, SPAN), SPAN)
        length = cols_ref[at, 2:3]
        value = act_s[at, head_lanes(1, head)]
        query = act_s[at, head_lanes(2, head)]
        key = act_s[at, head_lanes(3, head)]
        results = []
        for low, high in blocks:
            scores = dot(query[low:high], key[:high], 1, 1) * HEAD**-0.5
            keep = kept(low, high, length[low:high])
            attn = jnp.where(keep, scores * sigmoid(scores), 0.0).astype(BF16)
            results.append(dot(attn, value[:high]))
        att_s[at, head_lanes(0, head)] = jnp.concatenate(results, axis=0)
        return 0

    lax.fori_loop(0, 8, attend, 0, unroll=UNROLL)
    loads[2].wait()
    loads[3].wait()
    out_w = w_ref[:, 2560:3072]

    def middle(s, _):
        at = pl.ds(pl.multiple_of(s * SPAN, SPAN), SPAN)
        normed, scale = moments(att_s[at, :])
        gate = act_s[at, 0:512].astype(F32)
        gated = (normed * gate).astype(BF16)
        gated_s[at, :] = gated
        branch = dot(gated, out_w)
        out_ref[at, :] = (emb_s[at, :].astype(F32) + branch).astype(BF16)
        where = lax.broadcasted_iota(I32, (SPAN, 1), 0).astype(F32)
        grad = jnp.where(where < cols_ref[at, 2:3], cot_ref[at, :], jnp.zeros((), BF16))
        demb_s[at, :] = grad
        d_gated = dot(grad, out_w, 1, 1).astype(BF16).astype(F32)
        d_gate = (d_gated * normed).astype(BF16).astype(F32)
        dpre_s[at, 0:512] = (d_gate * slope_s[at, 0:512]).astype(BF16)
        datt_s[at, :] = norm_back(d_gated * gate, normed, scale).astype(BF16)
        return 0

    lax.fori_loop(0, 2, middle, 0)
    stores[3].start()
    g_ref[:, 2560:3072] = dot(gated_s[...], demb_s[...], 0, 0).astype(BF16)
    stores[2].start()

    def attend_back(i, _):
        s, head = i // 4, lax.rem(i, 4)
        at = pl.ds(pl.multiple_of(s * SPAN, SPAN), SPAN)
        length = cols_ref[at, 2:3]
        value = act_s[at, head_lanes(1, head)]
        query = act_s[at, head_lanes(2, head)]
        key = act_s[at, head_lanes(3, head)]
        d_att = datt_s[at, head_lanes(0, head)]
        d_query, d_key, d_value = [], [], []
        for low, high in blocks:
            scores = dot(query[low:high], key[:high], 1, 1) * HEAD**-0.5
            sig = sigmoid(scores)
            act = scores * sig
            keep = kept(low, high, length[low:high])
            attn = jnp.where(keep, act, 0.0).astype(BF16)
            d_attn = dot(d_att[low:high], value[:high], 1, 1).astype(BF16).astype(F32)
            slope = sig + act * (1.0 - sig)
            d_scores = (jnp.where(keep, d_attn * slope, 0.0) * HEAD**-0.5).astype(BF16)
            d_value.append(dot(attn, d_att[low:high], 0, 0))
            d_query.append(dot(d_scores, key[:high]))
            d_key.append(dot(d_scores, query[low:high], 0, 0))

        def whole(parts):
            return jnp.concatenate([parts[0] + parts[1][:256], parts[1][256:]], axis=0)

        grads = (whole(d_value), jnp.concatenate(d_query, axis=0), whole(d_key))
        for kind, grad in enumerate(grads):
            lanes = head_lanes(kind + 1, head)
            rounded = grad.astype(BF16).astype(F32)
            dpre_s[at, lanes] = (rounded * slope_s[at, lanes]).astype(BF16)
        return 0

    lax.fori_loop(0, 8, attend_back, 0, unroll=UNROLL)

    def first_weight(part, _):
        lanes = pl.ds(pl.multiple_of(part * 512, 512), 512)
        wide = pl.ds(pl.multiple_of(part * 512 + 512, 512), 512)
        g_ref[:, wide] = dot(norm_s[...], dpre_s[:, lanes], 0, 0).astype(BF16)
        return 0

    lax.fori_loop(0, 4, first_weight, 0)
    stores[1].start()

    def finish(s, _):
        at = pl.ds(pl.multiple_of(s * SPAN, SPAN), SPAN)
        d_normed = dot(dpre_s[at, 0:512], w_ref[:, 512:1024], 1, 1)
        for part in range(1, 4):
            lanes = slice(part * 512, part * 512 + 512)
            wide = slice(part * 512 + 512, part * 512 + 1024)
            d_normed = d_normed + dot(dpre_s[at, lanes], w_ref[:, wide], 1, 1)
        normed, scale = moments(emb_s[at, :].astype(F32))
        back = norm_back(d_normed.astype(BF16).astype(F32), normed, scale)
        d_emb = (demb_s[at, :].astype(F32) + back).astype(BF16)
        demb_s[at, :] = d_emb
        d_rows = dot(d_emb, proj, 1, 1)
        table = cols_ref[at, 1:2]
        rank = cols_ref[at, 3:4]
        lane = lax.broadcasted_iota(I32, (SPAN, half), 1)
        kind = jnp.where(lane < 64, 0.0, 1.0)
        for k in range(2):
            match = rank == float(k)
            low = k * 128
            place_s[at, low : low + 128] = jnp.where(
                (table == kind) & match, d_rows[:, 0:128], 0.0
            ).astype(BF16)
            place_s[at, 256 + low : 384 + low] = jnp.where(
                (table == 2.0) & match, d_rows[:, 128:256], 0.0
            ).astype(BF16)
            low = 512 + k * 256
            place_s[at, low : low + 256] = jnp.where(
                (table == 3.0) & match, d_rows[:, 256:512], 0.0
            ).astype(BF16)
        return 0

    lax.fori_loop(0, 2, finish, 0)
    g_ref[:, 0:512] = dot(rows_s[...], demb_s[...], 0, 0).astype(BF16)
    stores[0].start()
    owner = cols_ref[:, 0:1].astype(I32)
    hot = (owner == lax.broadcasted_iota(I32, (TOKENS, DEVICES), 1)).astype(BF16)
    first_ref[...] = dot(hot, place_s[:, 0:512], 0, 0).astype(BF16)
    second_ref[...] = dot(hot, place_s[:, 512:1024], 0, 0).astype(BF16)
    for copy in stores:
        copy.wait()


def layer(got, cols, weights, cotangent):
    def vmem(width, kind=BF16):
        return pltpu.VMEM((TOKENS, width), kind)

    return pl.pallas_call(
        layer_kernel,
        out_shape=(
            jax.ShapeDtypeStruct((TOKENS, WIDTH), BF16),
            jax.ShapeDtypeStruct((DEVICES, 512), BF16),
            jax.ShapeDtypeStruct((DEVICES, 512), BF16),
            jax.ShapeDtypeStruct((512, 3072), BF16),
        ),
        in_specs=[VM, VM, ANY, ANY],
        out_specs=(ANY, VM, VM, ANY),
        scratch_shapes=[
            vmem(512), vmem(512), vmem(512), vmem(2048, F32), vmem(2048), vmem(512, F32),
            vmem(512), vmem(512), vmem(2048), vmem(512), vmem(1024),
            pltpu.VMEM((512, 3072), BF16), vmem(512), vmem(512), pltpu.VMEM((512, 3072), BF16),
            pltpu.SemaphoreType.DMA((4,)), pltpu.SemaphoreType.DMA((4,)),
        ],
        compiler_params=pltpu.CompilerParams(vmem_limit_bytes=VMEM_LIMIT),
        name="layer",
    )(got, cols, weights, cotangent)


def scatter_kernel(
    got_ref, wanted_ref, total_ref, a_hbm, b_hbm, c_hbm, d_hbm, proj_ref, in_ref, out_ref,
    a_ref, b_ref, c_ref, d_ref, sem,
):
    stores = []
    proj_ref[...] = total_ref[:, 0:512].astype(F32)
    in_ref[...] = total_ref[:, 512:2560].astype(F32)
    out_ref[...] = total_ref[:, 2560:3072].astype(F32)
    row_form = wanted_ref[...]
    padded = jnp.concatenate([row_form, jnp.zeros((120, DEVICES), F32)], axis=0)
    col_form = jnp.transpose(padded)
    pairs = ((a_ref, a_hbm), (b_ref, b_hbm), (c_ref, c_hbm), (d_ref, d_hbm))
    for which, (grad_ref, grad_hbm) in enumerate(pairs):
        fold, rows = FOLD[which], ROWS[which]
        deep = rows // fold
        width = 256 // fold
        spread, inners = [], []
        for rank in range(2):
            row = col_form[:, rank * 4 + which : rank * 4 + which + 1].astype(I32)
            block = row // deep
            at = (0, 64, 256, 0)[which] + rank * (128, 128, 128, 256)[which]
            value = got_ref[which // 3, :, at : at + width].astype(F32)
            spread.append(
                jnp.concatenate([jnp.where(block == q, value, 0.0) for q in range(fold)], axis=1)
            )
            if which < 2:
                inners.append(row - block * deep)
            else:
                line = row_form[rank * 4 + which : rank * 4 + which + 1].astype(I32)
                inners.append(line - (line // deep) * deep)
        values = jnp.concatenate(spread, axis=0).astype(BF16)
        if which < 2:
            inner = jnp.concatenate(inners, axis=0)
            flipped = jnp.transpose(values.astype(F32)).astype(BF16)
            for at in range(0, deep, 512):
                hot = (inner == lax.broadcasted_iota(I32, (512, 512), 1) + at).astype(BF16)
                summed = dot(flipped, hot).astype(BF16)
                for q in range(fold):
                    grad_ref[:, q * deep + at : q * deep + at + 512] = summed[
                        q * width : (q + 1) * width
                    ]
        else:
            inner = jnp.concatenate(inners, axis=1)
            for at in range(0, deep, 512):
                hot = (inner == lax.broadcasted_iota(I32, (512, 512), 0) + at).astype(BF16)
                summed = dot(hot, values).astype(BF16)
                for q in range(fold):
                    grad_ref[q * deep + at : q * deep + at + 512, :] = summed[
                        :, q * width : (q + 1) * width
                    ]
        copy = pltpu.make_async_copy(grad_ref, grad_hbm, sem.at[which])
        copy.start()
        stores.append(copy)
    for copy in stores:
        copy.wait()


def scatter(got, wanted, totals):
    return pl.pallas_call(
        scatter_kernel,
        out_shape=(
            jax.ShapeDtypeStruct((64, ROWS[0]), BF16),
            jax.ShapeDtypeStruct((64, ROWS[1]), BF16),
            jax.ShapeDtypeStruct((ROWS[2], 128), BF16),
            jax.ShapeDtypeStruct((ROWS[3], 256), BF16),
            jax.ShapeDtypeStruct((16, 512), F32),
            jax.ShapeDtypeStruct((16, 2048), F32),
            jax.ShapeDtypeStruct((16, 512), F32),
        ),
        in_specs=[VM, VM, VM],
        out_specs=(ANY,) * 4 + (VM,) * 3,
        scratch_shapes=[
            pltpu.VMEM((64, ROWS[0]), BF16),
            pltpu.VMEM((64, ROWS[1]), BF16),
            pltpu.VMEM((ROWS[2], 128), BF16),
            pltpu.VMEM((ROWS[3], 256), BF16),
            pltpu.SemaphoreType.DMA((4,)),
        ],
        compiler_params=pltpu.CompilerParams(vmem_limit_bytes=VMEM_LIMIT),
        name="scatter",
    )(got, wanted, totals)


def add(*values):
    total = values[0].astype(F32)
    for value in values[1:]:
        total = total + value.astype(F32)
    return total


def deliver_kernel(
    first_ref, second_ref, g_ref, rows_ref, total_ref,
    across, pair, one, two, line, three, four, parts, column, mine, whole, *scratch,
):
    dp, xy, core, z = place()
    (x, right, left, to_right, to_left), (y, up, down, to_up, to_down) = near()
    far_x, far_y = lax.rem(x + 2, NX), lax.rem(y + 2, NY)
    link = Sender(*scratch[-2:])
    swap = Swap(link, first_ref, second_ref, rows_ref, *scratch[:-2])
    swap.ready_high()
    swap.ready_low()
    greet(swap.along_z + swap.along_dp)
    partner = peers()[2][0]
    start = link.start

    def meet(px, py, part):
        there = (px, py, 1 - core, part)
        return start(g_ref.at[there], across.at[px, py, part], partner)

    def join(px, py, part):
        for k in range(4):
            qx, qy = (px, k) if py is EVERY else (k, py)
            pair[qx, qy, part] = add(g_ref[qx, qy, core, part], across[qx, qy, part]).astype(BF16)

    far = [meet(far_x, EVERY, 0), meet(EVERY, far_y, 1)]
    high = swap.begin_high()
    sides = [
        meet(right, EVERY, 0), meet(left, EVERY, 0), meet(EVERY, up, 1), meet(EVERY, down, 1)
    ]
    centre = [meet(x, EVERY, 0), meet(EVERY, y, 1)]
    finish(far)
    join(far_x, EVERY, 0)
    join(EVERY, far_y, 1)
    steps = [
        start(pair.at[far_x, LOW, 0], one.at[0], to_right),
        start(pair.at[far_x, HIGH, 0], one.at[1], to_left),
        start(pair.at[LOW, far_y, 1], one.at[2], to_up),
        start(pair.at[HIGH, far_y, 1], one.at[3], to_down),
    ]
    low = swap.begin_low()
    finish(sides)
    join(right, EVERY, 0)
    join(left, EVERY, 0)
    join(EVERY, up, 1)
    join(EVERY, down, 1)
    finish(steps)
    for k in range(2):
        pair[right, k, 0] = add(pair[right, k, 0], one[0, k]).astype(BF16)
        pair[left, 2 + k, 0] = add(pair[left, 2 + k, 0], one[1, k]).astype(BF16)
        pair[k, up, 1] = add(pair[k, up, 1], one[2, k]).astype(BF16)
        pair[2 + k, down, 1] = add(pair[2 + k, down, 1], one[3, k]).astype(BF16)
    steps = [
        start(pair.at[right, :, 0], two.at[0], to_right),
        start(pair.at[left, :, 0], two.at[1], to_left),
        start(pair.at[:, up, 1], two.at[2], to_up),
        start(pair.at[:, down, 1], two.at[3], to_down),
    ]
    finish(low)
    low = swap.turn_low()
    finish(centre)
    join(x, EVERY, 0)
    join(EVERY, y, 1)
    finish(steps)
    for k in range(4):
        line[0, k] = add(pair[x, k, 0], two[0, k], two[1, k]).astype(BF16)
        line[1, k] = add(pair[k, y, 1], two[2, k], two[3, k]).astype(BF16)
    steps = [
        start(line.at[0, far_y, :, AHEAD], three.at[0], to_up),
        start(line.at[0, far_y, :, BEHIND], three.at[1], to_down),
        start(line.at[1, far_x, :, AHEAD], three.at[2], to_right),
        start(line.at[1, far_x, :, BEHIND], three.at[3], to_left),
    ]
    finish(high)
    high = swap.turn_high()
    finish(steps)
    line[0, up, :, AHEAD] = add(line[0, up, :, AHEAD], three[0]).astype(BF16)
    line[0, down, :, BEHIND] = add(line[0, down, :, BEHIND], three[1]).astype(BF16)
    line[1, right, :, AHEAD] = add(line[1, right, :, AHEAD], three[2]).astype(BF16)
    line[1, left, :, BEHIND] = add(line[1, left, :, BEHIND], three[3]).astype(BF16)
    finish(
        [
            start(line.at[0, up], four.at[0], to_up),
            start(line.at[0, down], four.at[1], to_down),
            start(line.at[1, right], four.at[2], to_right),
            start(line.at[1, left], four.at[3], to_left),
        ]
    )
    for q in range(NZ):
        lanes = pl.ds(q * 384, 384)
        parts[q, 0] = add(line[0, y, :, lanes], four[0, :, lanes], four[1, :, lanes]).astype(BF16)
        parts[q, 1] = add(line[1, x, :, lanes], four[2, :, lanes], four[3, :, lanes]).astype(BF16)
    steps = [start(parts.at[t[1]], column.at[i], t) for i, t in enumerate(swap.along_z)]
    finish(low)
    swap.end_low()
    finish(steps)
    mine[...] = add(parts[z], *[column[k] for k in range(NZ - 1)]).astype(BF16)
    steps = [start(mine, whole.at[z], t) for t in swap.along_z]
    whole[pl.ds(z, 1)] = mine[...][None]
    finish(high + steps)
    for half in range(2):
        for q in range(NZ):
            total_ref[half * 8 : half * 8 + 8, q * 384 : q * 384 + 384] = whole[q, half]


def deliver(first, second, terms):
    return pl.pallas_call(
        deliver_kernel,
        out_shape=(
            jax.ShapeDtypeStruct((2, 32, 8, 512), BF16),
            jax.ShapeDtypeStruct((16, 3072), BF16),
        ),
        in_specs=[VM] * 3,
        out_specs=(VM, VM),
        scratch_shapes=[
            pltpu.VMEM((4, 4, 2, 8, 3072), BF16),
            pltpu.VMEM((4, 4, 2, 8, 3072), BF16),
            pltpu.VMEM((4, 2, 8, 3072), BF16),
            pltpu.VMEM((4, 4, 8, 3072), BF16),
            pltpu.VMEM((2, 4, 8, 3072), BF16),
            pltpu.VMEM((4, 8, 1536), BF16),
            pltpu.VMEM((4, 8, 3072), BF16),
            pltpu.VMEM((8, 2, 8, 384), BF16),
            pltpu.VMEM((7, 2, 8, 384), BF16),
            pltpu.VMEM((2, 8, 384), BF16),
            pltpu.VMEM((8, 2, 8, 384), BF16),
        ]
        + SWAP_SHAPES
        + sems(114),
        compiler_params=comm_params(3),
        name="deliver",
    )(first, second, terms)


def shards(
    item_ids, table_ids, lengths, assignment,
    table_a, table_b, table_c, table_d,
    proj_weight, in_weight, out_weight, cotangent,
):
    got, full, wanted, cols = front(
        item_ids,
        table_ids,
        lengths,
        assignment,
        (proj_weight, in_weight, out_weight),
        (table_a.T, table_b.T, table_c, table_d),
    )
    output, first, second, terms = layer(
        got.reshape(2, DEVICES, 512),
        cols,
        full.reshape(512, 3072),
        cotangent.reshape(TOKENS, WIDTH),
    )
    arrived, totals = deliver(
        first, second.reshape(32, 8, 512), terms.reshape(NX, NY, 2, 2, 8, 3072)
    )
    grads = scatter(arrived.reshape(2, DEVICES, 512), wanted, totals)
    return (
        output.reshape(2, SPAN, WIDTH),
        grads[0].T,
        grads[1].T,
        *grads[2:],
    )


def solution(mesh):
    both = ("dp", "table")
    return jax.shard_map(
        shards,
        mesh=mesh,
        in_specs=(
            P(both, None), P(both, None), P(both), P(both),
            P(both, None), P(both, None), P(both, None), P(both, None),
            P("dp", None), P("dp", None), P("dp", None), P(both, None, None),
        ),
        out_specs=(
            P(both, None, None),
            P(both, None), P(both, None), P(both, None), P(both, None),
            P("dp", None), P("dp", None), P("dp", None),
        ),
        check_vma=False,
    )
```

```python
import functools

import jax
import jax.numpy as jnp
from jax import lax
from jax.experimental import pallas as pl
from jax.experimental.pallas import tpu as pltpu
from jax.sharding import PartitionSpec as P

MESH = pl.DeviceIdType.MESH
VM = pl.BlockSpec(memory_space=pltpu.VMEM)
F32, BF16, I32 = jnp.float32, jnp.bfloat16, jnp.int32
NX, NY, NZ, PLANE = 4, 4, 8, 16
DEVICES = 256
HEADS, HEAD = 4, 128
SPAN, TOKENS, WIDTH = 384, 768, 512
ROWS = (12288, 12288, 6144, 2048)
FOLD = (4, 4, 2, 1)
TABLE_BITS = 22
KEY = 1024
NONE = 16383.0 * KEY
VMEM_LIMIT = 60 << 20
UNROLL = 4
ANY = pl.BlockSpec(memory_space=pl.ANY)


def place():
    dp, z = lax.axis_index("dp"), lax.axis_index("table")
    return dp, dp // 2, lax.rem(dp, 2), z


def plane_peer(xy, k):
    x = lax.rem(xy // NY + k // NY, NX)
    y = lax.rem(lax.rem(xy, NY) + k % NY, NY)
    return x * NY + y


def peers():
    dp, xy, core, z = place()
    along_z = [(dp, lax.rem(z + k, NZ)) for k in range(1, NZ)]
    in_plane = [(plane_peer(xy, k) * 2 + core, z) for k in range(1, PLANE)]
    return along_z, in_plane, [(xy * 2 + (1 - core), z)]


def near():
    dp, xy, core, z = place()
    x, y = xy // NY, lax.rem(xy, NY)
    right, left = lax.rem(x + 1, NX), lax.rem(x + NX - 1, NX)
    up, down = lax.rem(y + 1, NY), lax.rem(y + NY - 1, NY)

    def at(px, py):
        return ((px * NY + py) * 2 + core, z)

    return (x, right, left, at(right, y), at(left, y)), (y, up, down, at(x, up), at(x, down))


def knock(targets):
    barrier = pltpu.get_barrier_semaphore()
    for dp, z in targets:
        pl.semaphore_signal(barrier, inc=1, device_id=(dp, z), device_id_type=MESH)


def admit(targets):
    pl.semaphore_wait(pltpu.get_barrier_semaphore(), len(targets))


def greet(targets):
    knock(targets)
    admit(targets)


def send(src, dst, send_sem, recv_sem, target):
    copy = pltpu.make_async_remote_copy(
        src_ref=src,
        dst_ref=dst,
        send_sem=send_sem,
        recv_sem=recv_sem,
        device_id=target,
        device_id_type=MESH,
    )
    copy.start()
    return copy


def dot(a, b, da=1, db=0):
    return lax.dot_general(a, b, (((da,), (db,)), ((), ())), preferred_element_type=F32)


class Sender:
    def __init__(self, send_sem, recv_sem):
        self.sems, self.used = (send_sem, recv_sem), 0

    def start(self, src, dst, target):
        at, self.used = self.used, self.used + 1
        return send(src, dst, self.sems[0].at[at], self.sems[1].at[at], target)

    def move(self, ref, target):
        return self.start(ref, ref, target)


def finish(copies):
    for copy in copies:
        copy.wait()


EVERY, LOW, HIGH = slice(None), pl.ds(0, 2), pl.ds(2, 2)
AHEAD, BEHIND = pl.ds(0, 1536), pl.ds(1536, 1536)


def sems(count):
    return [pltpu.SemaphoreType.DMA((count,)), pltpu.SemaphoreType.DMA((count,))]


def comm_params(collective):
    return pltpu.CompilerParams(
        collective_id=collective, has_side_effects=True, vmem_limit_bytes=VMEM_LIMIT
    )


SM = pl.BlockSpec(memory_space=pltpu.SMEM)


class Swap:
    def __init__(self, link, first_ref, second_ref, out_ref, by_z, from_z, by_dp, from_dp, again_z, from_z2):
        self.link, self.first, self.second, self.out = link, first_ref, second_ref, out_ref
        self.by_z, self.from_z, self.by_dp = by_z, from_z, by_dp
        self.from_dp, self.again_z, self.from_z2 = from_dp, again_z, from_z2
        self.dp, xy, core, self.z = place()
        self.along_z, in_plane, partner = peers()
        others = [(plane_peer(xy, k) * 2 + (1 - core), self.z) for k in range(1, PLANE)]
        self.along_dp = in_plane + partner + others
        i = lax.broadcasted_iota(I32, (DEVICES, DEVICES), 0)
        j = lax.broadcasted_iota(I32, (DEVICES, DEVICES), 1)
        self.z_first = (j == (i & 31) * 8 + (i >> 5)).astype(BF16)
        self.dp_first = (j == (i & 7) * 32 + (i >> 3)).astype(BF16)

    def ready_high(self):
        self.by_z[...] = self.arrange(self.z_first, self.first, (NZ, 32, 512))
        self.from_z[pl.ds(self.z, 1)] = self.by_z[pl.ds(self.z, 1)]

    def ready_low(self):
        self.from_dp[pl.ds(self.dp, 1)] = self.second[pl.ds(self.dp, 1)]

    def arrange(self, matrix, ref, dims):
        return dot(matrix, ref[...].reshape(DEVICES, 512)).astype(BF16).reshape(dims)

    def begin_high(self):
        return [self.link.start(self.by_z.at[t[1]], self.from_z.at[self.z], t) for t in self.along_z]

    def begin_low(self):
        return [
            self.link.start(self.second.at[t[0]], self.from_dp.at[self.dp], t)
            for t in self.along_dp
        ]

    def turn_low(self):
        self.again_z[...] = self.arrange(self.z_first, self.from_dp, (NZ, 32, 512))
        self.from_z2[pl.ds(self.z, 1)] = self.again_z[pl.ds(self.z, 1)]
        return [
            self.link.start(self.again_z.at[t[1]], self.from_z2.at[self.z], t)
            for t in self.along_z
        ]

    def turn_high(self):
        self.by_dp[...] = self.arrange(self.dp_first, self.from_z, (32, NZ, 512))
        self.out[0, pl.ds(self.dp, 1)] = self.by_dp[pl.ds(self.dp, 1)]
        return [
            self.link.start(self.by_dp.at[t[0]], self.out.at[0, self.dp], t) for t in self.along_dp
        ]

    def end_low(self):
        self.out[1] = self.arrange(self.dp_first, self.from_z2, (32, NZ, 512))


SWAP_SHAPES = [
    pltpu.VMEM((8, 32, 512), BF16),
    pltpu.VMEM((8, 32, 512), BF16),
    pltpu.VMEM((32, 8, 512), BF16),
    pltpu.VMEM((32, 8, 512), BF16),
    pltpu.VMEM((8, 32, 512), BF16),
    pltpu.VMEM((8, 32, 512), BF16),
]


def smallest_two(keys):
    first = jnp.full((8, keys.shape[1]), NONE, F32)
    second = first
    for at in range(0, keys.shape[0], 8):
        value = keys[at : at + 8]
        second = jnp.minimum(second, jnp.maximum(first, value))
        first = jnp.minimum(first, value)
    low = jnp.min(first, axis=0, keepdims=True)
    high = jnp.min(jnp.where(first == low, second, first), axis=0, keepdims=True)
    return low, high


def front_kernel(
    items_ref, tables_ref, lengths_ref, targets_ref, proj_ref, in_ref, wout_ref,
    a_hbm, b_hbm, c_hbm, d_hbm,
    out_ref, full_ref, wanted_ref, cols_ref,
    ids_ref, moved, first_ref, second_ref, a_ref, b_ref, c_ref, d_ref, sem, *scratch,
):
    *buffers, send_sem, recv_sem = scratch
    hbm, tables = (a_hbm, b_hbm, c_hbm, d_hbm), (a_ref, b_ref, c_ref, d_ref)
    loads = [pltpu.make_async_copy(hbm[i], tables[i], sem.at[i]) for i in range(4)]
    for copy in loads:
        copy.start()
    dp, xy, core, z = place()
    me = dp * NZ + z
    (x, right, left, to_right, to_left), (y, up, down, to_up, to_down) = near()
    far_x, far_y = lax.rem(x + 2, NX), lax.rem(y + 2, NY)
    to_far_x, to_far_y = ((far_x * NY + y) * 2 + core, z), ((x * NY + far_y) * 2 + core, z)
    lane = lax.broadcasted_iota(I32, (1, 128), 1)
    events = tables_ref[...] * (1 << TABLE_BITS) + items_ref[...]
    lines = []
    for s in range(2):
        lines += [events[s : s + 1, r * 128 : r * 128 + 128] for r in range(3)]
        lines.append(jnp.where(lane == 0, lengths_ref[s], jnp.where(lane == 1, targets_ref[s], 0)))
    ids_ref[x, y, core, z] = jnp.concatenate(lines, axis=0)
    for half in range(2):
        rows = slice(half * 8, half * 8 + 8)
        full_ref[x, y, core, half, :, 0:512] = proj_ref[rows, :]
        full_ref[x, y, core, half, :, 512:2560] = in_ref[rows, :]
        full_ref[x, y, core, half, :, 2560:3072] = wout_ref[rows, :]
    along_z, _plane, partner = peers()
    partner = partner[0]
    near_x, near_y = [to_right, to_left], [to_up, to_down]
    link = Sender(send_sem, recv_sem)
    swap = Swap(link, first_ref, second_ref, out_ref, *buffers)
    greet(swap.along_z + swap.along_dp)

    def ids(px, py, low):
        return ids_ref.at[px, py, core, pl.ds(low, 4)]

    def w(px, py, part):
        return full_ref.at[px, py, core, part]

    own = ids_ref.at[x, y, core, z]
    one = [link.move(own, t) for t in along_z]
    w_one = [link.move(w(x, y, 0), t) for t in near_y] + [link.move(w(x, y, 1), t) for t in near_x]
    finish(one)
    two = [link.move(ids(x, y, 0), t) for t in near_y + [to_far_y]]
    two += [link.move(ids(x, y, 4), t) for t in near_x + [to_far_x]]
    finish(w_one)
    w_two = [
        link.move(full_ref.at[x, down, core, 0, :, AHEAD], to_up),
        link.move(full_ref.at[x, up, core, 0, :, BEHIND], to_down),
        link.move(full_ref.at[left, y, core, 1, :, AHEAD], to_right),
        link.move(full_ref.at[right, y, core, 1, :, BEHIND], to_left),
    ]
    finish(two)
    three = [link.move(ids(x, EVERY, 0), t) for t in [to_far_x] + near_x]
    three += [link.move(ids(EVERY, y, 4), t) for t in [to_far_y] + near_y]
    across = [link.move(ids(x, EVERY, 0), partner), link.move(ids(EVERY, y, 4), partner)]
    finish(w_two)
    w_three = [
        link.move(w(x, EVERY, 0), to_right),
        link.move(w(x, EVERY, 0), to_left),
        link.move(w(EVERY, y, 1), to_up),
        link.move(w(EVERY, y, 1), to_down),
    ]
    w_across = [link.move(w(x, EVERY, 0), partner), link.move(w(EVERY, y, 1), partner)]
    finish(three)
    across += [link.move(ids(side, EVERY, 0), partner) for side in (right, left, far_x)]
    across += [link.move(ids(EVERY, side, 4), partner) for side in (up, down, far_y)]
    finish(across)

    def line_of(j):
        return ids_ref[:, :, :, :, j, :].reshape(DEVICES, 128)

    words = jnp.concatenate(
        [
            jnp.concatenate([line_of(4 * s + r) for r in range(3)], axis=1)
            for s in range(2)
        ],
        axis=0,
    )
    extra = jnp.concatenate([line_of(3), line_of(7)], axis=0)
    lengths = extra[:, 0:1].astype(F32)
    targets = extra[:, 1:2]
    arranged = (targets & 1) * DEVICES + (targets >> 1)
    slots = lax.broadcasted_iota(I32, (512, 512), 1)
    goes = (arranged == slots).astype(BF16)
    total = None
    for shift in (16, 8, 0):
        part = ((words >> shift) & 255).astype(F32).astype(BF16)
        piece = dot(part, goes, 0, 0)
        total = piece if total is None else total * 256.0 + piece
    moved[...] = total

    place_of = lax.broadcasted_iota(I32, (SPAN, 512), 0).astype(F32)
    lows, highs = [], []
    for which in range(4):
        start = which * (1 << TABLE_BITS) + me * ROWS[which]
        local = moved[...] - start.astype(F32)
        held = (local >= 0.0) & (local < float(ROWS[which]))
        keys = jnp.where(held, local * float(KEY) + place_of, NONE)
        low, high = smallest_two(keys)
        low_a, high_a = low[:, :DEVICES], high[:, :DEVICES]
        low_b, high_b = low[:, DEVICES:] + float(SPAN), high[:, DEVICES:] + float(SPAN)
        lows.append(jnp.minimum(low_a, low_b))
        highs.append(jnp.minimum(jnp.maximum(low_a, low_b), jnp.minimum(high_a, high_b)))
    row_form = jnp.floor(jnp.concatenate(lows + highs, axis=0) * (1.0 / KEY))
    wanted_ref[...] = row_form
    padded = jnp.concatenate([row_form, jnp.zeros((120, DEVICES), F32)], axis=0)
    col_form = jnp.transpose(padded)

    def find(which):
        table_ref = tables[which]
        loads[which].wait()
        fold, rows = FOLD[which], ROWS[which]
        deep = rows // fold
        width = 256 // fold
        for rank in range(2):
            row = col_form[:, rank * 4 + which : rank * 4 + which + 1].astype(I32)
            block = row // deep
            inner = row - block * deep
            acc = jnp.zeros((DEVICES, 256), F32)
            tile = 1024
            for at in range(0, deep, tile):
                index = lax.broadcasted_iota(I32, (DEVICES, tile), 1) + at
                hot = (inner == index).astype(BF16)
                if which < 2:
                    piece = jnp.concatenate(
                        [table_ref[:, q * deep + at : q * deep + at + tile] for q in range(fold)],
                        axis=0,
                    )
                    acc = acc + dot(hot, piece, 1, 1)
                else:
                    piece = jnp.concatenate(
                        [table_ref[q * deep + at : q * deep + at + tile, :] for q in range(fold)],
                        axis=1,
                    )
                    acc = acc + dot(hot, piece)
            value = jnp.zeros((DEVICES, width), F32)
            for q in range(fold):
                value = value + jnp.where(block == q, acc[:, q * width : (q + 1) * width], 0.0)
            at = (0, 64, 256, 0)[which] + rank * (128, 128, 128, 256)[which]
            if which == 3:
                second_ref[:, :, at : at + width] = value.astype(BF16).reshape(32, NZ, width)
            else:
                first_ref[:, at : at + width] = value.astype(BF16)

    find(3)
    swap.ready_low()
    low = swap.begin_low()
    finish(w_three)
    w_four = [
        link.move(w(left, LOW, 0), to_right),
        link.move(w(right, HIGH, 0), to_left),
        link.move(w(LOW, down, 1), to_up),
        link.move(w(HIGH, up, 1), to_down),
    ]
    w_across += [link.move(w(side, EVERY, 0), partner) for side in (right, left)]
    w_across += [link.move(w(EVERY, side, 1), partner) for side in (up, down)]
    for which in range(3):
        find(which)
    swap.ready_high()
    high = swap.begin_high()
    finish(low)
    low = swap.turn_low()
    finish(w_four)
    w_across += [link.move(w(far_x, EVERY, 0), partner), link.move(w(EVERY, far_y, 1), partner)]

    pieces, spans = [], []
    for s in range(2):
        hit = targets == 2 * me + s
        pieces.append(jnp.sum(jnp.where(hit, words, 0), axis=0, keepdims=True))
        length = jnp.sum(jnp.where(hit, lengths, 0.0), axis=0, keepdims=True)
        spans.append(jnp.broadcast_to(length, (1, SPAN)))
    event = jnp.concatenate(pieces, axis=1)
    span = jnp.concatenate(spans, axis=1)
    table = event >> TABLE_BITS
    item = event & ((1 << TABLE_BITS) - 1)
    unit = jnp.where(table == 3, item >> 11, jnp.where(table == 2, item >> 11, item >> 12))
    third = jnp.floor((unit.astype(F32) + 0.5) * (1.0 / 3.0)).astype(I32)
    owner = jnp.where(table == 3, unit, third)
    per = jnp.where(table == 3, ROWS[3], jnp.where(table == 2, ROWS[2], ROWS[0]))
    local = item - owner * per
    order = lax.broadcasted_iota(I32, (1, TOKENS), 1)
    key = (local * KEY + order).astype(F32)
    bucket = (table * DEVICES + owner).astype(F32)
    lines = [owner.astype(F32), table.astype(F32), span, key, bucket]
    stacked = jnp.concatenate(lines + [jnp.zeros((123, TOKENS), F32)], axis=0)
    cols = jnp.transpose(stacked)
    ahead = (cols[:, 4:5] == bucket) & (key < cols[:, 3:4])
    rank = jnp.sum(jnp.where(ahead, 1.0, 0.0), axis=1, keepdims=True)
    lane = lax.broadcasted_iota(I32, (TOKENS, 128), 1)
    cols_ref[...] = jnp.where(lane == 3, rank, cols)

    finish(high)
    high = swap.turn_high()
    finish(low)
    swap.end_low()
    finish(high + w_across)


def front(items, tables, lengths, targets, weights, held):
    return pl.pallas_call(
        front_kernel,
        out_shape=(
            jax.ShapeDtypeStruct((2, 32, 8, 512), BF16),
            jax.ShapeDtypeStruct((NX, NY, 2, 2, 8, 3072), BF16),
            jax.ShapeDtypeStruct((8, DEVICES), F32),
            jax.ShapeDtypeStruct((TOKENS, 128), F32),
        ),
        in_specs=[VM, VM, SM, SM, VM, VM, VM] + [ANY] * 4,
        out_specs=(VM,) * 4,
        scratch_shapes=[
            pltpu.VMEM((NX, NY, 2, NZ, 8, 128), I32),
            pltpu.VMEM((SPAN, 512), F32),
            pltpu.VMEM((DEVICES, 512), BF16),
            pltpu.VMEM((32, NZ, 512), BF16),
            pltpu.VMEM((64, ROWS[0]), BF16),
            pltpu.VMEM((64, ROWS[1]), BF16),
            pltpu.VMEM((ROWS[2], 128), BF16),
            pltpu.VMEM((ROWS[3], 256), BF16),
            pltpu.SemaphoreType.DMA((4,)),
        ]
        + SWAP_SHAPES
        + sems(127),
        compiler_params=comm_params(1),
        name="front",
    )(items, tables, lengths, targets, *weights, *held)


def moments(values):
    mean = jnp.mean(values, axis=-1, keepdims=True)
    centred = values - mean
    scale = lax.rsqrt(jnp.mean(centred * centred, axis=-1, keepdims=True) + 1e-05)
    return centred * scale, scale


def norm_back(grad, normed, scale):
    inner = jnp.mean(grad * normed, axis=-1, keepdims=True)
    return scale * (grad - jnp.mean(grad, axis=-1, keepdims=True) - normed * inner)


def sigmoid(values):
    return 0.5 * jnp.tanh(0.5 * values) + 0.5


def scatter_kernel(
    got_ref, wanted_ref, total_ref, a_hbm, b_hbm, c_hbm, d_hbm, proj_ref, in_ref, out_ref,
    a_ref, b_ref, c_ref, d_ref, sem,
):
    stores = []
    proj_ref[...] = total_ref[:, 0:512].astype(F32)
    in_ref[...] = total_ref[:, 512:2560].astype(F32)
    out_ref[...] = total_ref[:, 2560:3072].astype(F32)
    row_form = wanted_ref[...]
    padded = jnp.concatenate([row_form, jnp.zeros((120, DEVICES), F32)], axis=0)
    col_form = jnp.transpose(padded)
    pairs = ((a_ref, a_hbm), (b_ref, b_hbm), (c_ref, c_hbm), (d_ref, d_hbm))
    for which, (grad_ref, grad_hbm) in enumerate(pairs):
        fold, rows = FOLD[which], ROWS[which]
        deep = rows // fold
        width = 256 // fold
        spread, inners = [], []
        for rank in range(2):
            row = col_form[:, rank * 4 + which : rank * 4 + which + 1].astype(I32)
            block = row // deep
            at = (0, 64, 256, 0)[which] + rank * (128, 128, 128, 256)[which]
            value = got_ref[which // 3, :, at : at + width].astype(F32)
            spread.append(
                jnp.concatenate([jnp.where(block == q, value, 0.0) for q in range(fold)], axis=1)
            )
            if which < 2:
                inners.append(row - block * deep)
            else:
                line = row_form[rank * 4 + which : rank * 4 + which + 1].astype(I32)
                inners.append(line - (line // deep) * deep)
        values = jnp.concatenate(spread, axis=0).astype(BF16)
        if which < 2:
            inner = jnp.concatenate(inners, axis=0)
            flipped = jnp.transpose(values.astype(F32)).astype(BF16)
            for at in range(0, deep, 512):
                hot = (inner == lax.broadcasted_iota(I32, (512, 512), 1) + at).astype(BF16)
                summed = dot(flipped, hot).astype(BF16)
                for q in range(fold):
                    grad_ref[:, q * deep + at : q * deep + at + 512] = summed[
                        q * width : (q + 1) * width
                    ]
        else:
            inner = jnp.concatenate(inners, axis=1)
            for at in range(0, deep, 512):
                hot = (inner == lax.broadcasted_iota(I32, (512, 512), 0) + at).astype(BF16)
                summed = dot(hot, values).astype(BF16)
                for q in range(fold):
                    grad_ref[q * deep + at : q * deep + at + 512, :] = summed[
                        :, q * width : (q + 1) * width
                    ]
        copy = pltpu.make_async_copy(grad_ref, grad_hbm, sem.at[which])
        copy.start()
        stores.append(copy)
    for copy in stores:
        copy.wait()


def scatter(got, wanted, totals):
    return pl.pallas_call(
        scatter_kernel,
        out_shape=(
            jax.ShapeDtypeStruct((64, ROWS[0]), BF16),
            jax.ShapeDtypeStruct((64, ROWS[1]), BF16),
            jax.ShapeDtypeStruct((ROWS[2], 128), BF16),
            jax.ShapeDtypeStruct((ROWS[3], 256), BF16),
            jax.ShapeDtypeStruct((16, 512), F32),
            jax.ShapeDtypeStruct((16, 2048), F32),
            jax.ShapeDtypeStruct((16, 512), F32),
        ),
        in_specs=[VM, VM, VM],
        out_specs=(ANY,) * 4 + (VM,) * 3,
        scratch_shapes=[
            pltpu.VMEM((64, ROWS[0]), BF16),
            pltpu.VMEM((64, ROWS[1]), BF16),
            pltpu.VMEM((ROWS[2], 128), BF16),
            pltpu.VMEM((ROWS[3], 256), BF16),
            pltpu.SemaphoreType.DMA((4,)),
        ],
        compiler_params=pltpu.CompilerParams(vmem_limit_bytes=VMEM_LIMIT),
        name="scatter",
    )(got, wanted, totals)


def add(*values):
    total = values[0].astype(F32)
    for value in values[1:]:
        total = total + value.astype(F32)
    return total


def core_kernel(
    got_ref, cols_ref, w_hbm, cot_hbm, out_hbm, row_ref, total_ref,
    rows_s, emb_s, norm_s, slope_s, act_s, att_s, gated_s, datt_s, dpre_s, demb_s, place_s,
    w_ref, cot_ref, out_ref, in_sem, out_sem, first_ref, second_ref, g_ref,
    across, pair, one, two, line, three, four, parts, column, mine, whole, *scratch,
):
    dp, xy, core, z = place()
    (x, right, left, to_right, to_left), (y, up, down, to_up, to_down) = near()
    far_x, far_y = lax.rem(x + 2, NX), lax.rem(y + 2, NY)
    link = Sender(*scratch[-2:])
    swap = Swap(link, first_ref, second_ref, row_ref, *scratch[:-2])
    partner = peers()[2][0]
    start = link.start
    everyone = swap.along_z + swap.along_dp
    knock(everyone)
    half = 128
    pieces = (slice(0, 512), slice(512, 2560), slice(2560, 3072))
    loads = [
        pltpu.make_async_copy(w_hbm.at[:, part], w_ref.at[:, part], in_sem.at[i])
        for i, part in enumerate(pieces)
    ]
    loads.append(pltpu.make_async_copy(cot_hbm, cot_ref, in_sem.at[3]))
    for copy in loads:
        copy.start()
    store = pltpu.make_async_copy(out_ref, out_hbm, out_sem)

    def term(value):
        return value.reshape(NX, NY, 2, 2, 8, 512).astype(BF16)

    loads[0].wait()
    proj = w_ref[:, 0:512]

    def begin(s, _):
        at = pl.ds(pl.multiple_of(s * SPAN, SPAN), SPAN)
        owner = cols_ref[at, 0:1].astype(I32)
        table = cols_ref[at, 1:2]
        rank = cols_ref[at, 3:4]
        hot = (owner == lax.broadcasted_iota(I32, (SPAN, DEVICES), 1)).astype(BF16)
        lane = lax.broadcasted_iota(I32, (SPAN, half), 1)
        kind = jnp.where(lane < 64, 0.0, 1.0)
        got = dot(hot, got_ref[0])
        first = rank == 0.0
        ab = jnp.where((table == kind), jnp.where(first, got[:, 0:128], got[:, 128:256]), 0.0)
        c = jnp.where(table == 2.0, jnp.where(first, got[:, 256:384], got[:, 384:512]), 0.0)
        got = dot(hot, got_ref[1])
        d = jnp.where(table == 3.0, jnp.where(first, got[:, 0:256], got[:, 256:512]), 0.0)
        rows = jnp.concatenate([ab, c, d], axis=1).astype(BF16)
        rows_s[at, :] = rows
        emb = dot(rows, proj).astype(BF16)
        emb_s[at, :] = emb
        normed, _scale = moments(emb.astype(F32))
        norm_s[at, :] = normed.astype(BF16)
        return 0

    lax.fori_loop(0, 2, begin, 0)

    loads[1].wait()

    def project(i, _):
        s, part = i // 4, lax.rem(i, 4)
        at = pl.ds(pl.multiple_of(s * SPAN, SPAN), SPAN)
        lanes = pl.ds(pl.multiple_of(part * 512, 512), 512)
        pre = dot(norm_s[at, :], w_ref[:, pl.ds(pl.multiple_of(part * 512 + 512, 512), 512)])
        sig = sigmoid(pre)
        act = pre * sig
        slope_s[at, lanes] = sig + act * (1.0 - sig)
        act_s[at, lanes] = act.astype(BF16)
        return 0

    lax.fori_loop(0, 8, project, 0)

    blocks = ((0, 256), (256, 384))

    def head_lanes(kind, head):
        return pl.ds(pl.multiple_of(kind * 512 + head * HEAD, HEAD), HEAD)

    def kept(low, high, length):
        row = lax.broadcasted_iota(I32, (high - low, high), 0) + low
        column = lax.broadcasted_iota(I32, (high - low, high), 1)
        return (column <= row) & (column.astype(F32) < length)

    def attend(i, _):
        s, head = i // 4, lax.rem(i, 4)
        at = pl.ds(pl.multiple_of(s * SPAN, SPAN), SPAN)
        length = cols_ref[at, 2:3]
        value = act_s[at, head_lanes(1, head)]
        query = act_s[at, head_lanes(2, head)]
        key = act_s[at, head_lanes(3, head)]
        results = []
        for low, high in blocks:
            scores = dot(query[low:high], key[:high], 1, 1) * HEAD**-0.5
            keep = kept(low, high, length[low:high])
            attn = jnp.where(keep, scores * sigmoid(scores), 0.0).astype(BF16)
            results.append(dot(attn, value[:high]))
        att_s[at, head_lanes(0, head)] = jnp.concatenate(results, axis=0)
        return 0

    lax.fori_loop(0, 8, attend, 0, unroll=UNROLL)
    loads[2].wait()
    loads[3].wait()
    out_w = w_ref[:, 2560:3072]

    def middle(s, _):
        at = pl.ds(pl.multiple_of(s * SPAN, SPAN), SPAN)
        normed, scale = moments(att_s[at, :])
        gate = act_s[at, 0:512].astype(F32)
        gated = (normed * gate).astype(BF16)
        gated_s[at, :] = gated
        branch = dot(gated, out_w)
        out_ref[at, :] = (emb_s[at, :].astype(F32) + branch).astype(BF16)
        where = lax.broadcasted_iota(I32, (SPAN, 1), 0).astype(F32)
        grad = jnp.where(where < cols_ref[at, 2:3], cot_ref[at, :], jnp.zeros((), BF16))
        demb_s[at, :] = grad
        d_gated = dot(grad, out_w, 1, 1).astype(BF16).astype(F32)
        d_gate = (d_gated * normed).astype(BF16).astype(F32)
        dpre_s[at, 0:512] = (d_gate * slope_s[at, 0:512]).astype(BF16)
        datt_s[at, :] = norm_back(d_gated * gate, normed, scale).astype(BF16)
        return 0

    lax.fori_loop(0, 2, middle, 0)
    store.start()
    g_ref[:, :, :, :, :, 2560:3072] = term(dot(gated_s[...], demb_s[...], 0, 0))

    def attend_back(i, _):
        s, head = i // 4, lax.rem(i, 4)
        at = pl.ds(pl.multiple_of(s * SPAN, SPAN), SPAN)
        length = cols_ref[at, 2:3]
        value = act_s[at, head_lanes(1, head)]
        query = act_s[at, head_lanes(2, head)]
        key = act_s[at, head_lanes(3, head)]
        d_att = datt_s[at, head_lanes(0, head)]
        d_query, d_key, d_value = [], [], []
        for low, high in blocks:
            scores = dot(query[low:high], key[:high], 1, 1) * HEAD**-0.5
            sig = sigmoid(scores)
            act = scores * sig
            keep = kept(low, high, length[low:high])
            attn = jnp.where(keep, act, 0.0).astype(BF16)
            d_attn = dot(d_att[low:high], value[:high], 1, 1).astype(BF16).astype(F32)
            slope = sig + act * (1.0 - sig)
            d_scores = (jnp.where(keep, d_attn * slope, 0.0) * HEAD**-0.5).astype(BF16)
            d_value.append(dot(attn, d_att[low:high], 0, 0))
            d_query.append(dot(d_scores, key[:high]))
            d_key.append(dot(d_scores, query[low:high], 0, 0))

        def whole(parts):
            return jnp.concatenate([parts[0] + parts[1][:256], parts[1][256:]], axis=0)

        grads = (whole(d_value), jnp.concatenate(d_query, axis=0), whole(d_key))
        for kind, grad in enumerate(grads):
            lanes = head_lanes(kind + 1, head)
            rounded = grad.astype(BF16).astype(F32)
            dpre_s[at, lanes] = (rounded * slope_s[at, lanes]).astype(BF16)
        return 0

    lax.fori_loop(0, 8, attend_back, 0, unroll=UNROLL)

    def first_weight(part, _):
        lanes = pl.ds(pl.multiple_of(part * 512, 512), 512)
        wide = pl.ds(pl.multiple_of(part * 512 + 512, 512), 512)
        g_ref[:, :, :, :, :, wide] = term(dot(norm_s[...], dpre_s[:, lanes], 0, 0))
        return 0

    lax.fori_loop(0, 4, first_weight, 0)
    late, early = pl.ds(0, 512), pl.ds(512, 2560)

    def meet(px, py, part, lanes):
        source = g_ref.at[px, py, 1 - core, part, :, lanes]
        return start(source, across.at[px, py, part, :, lanes], partner)

    def meet_all(lanes):
        far = [meet(far_x, EVERY, 0, lanes), meet(EVERY, far_y, 1, lanes)]
        rest = [meet(side, EVERY, 0, lanes) for side in (right, left, x)]
        return far, rest + [meet(EVERY, side, 1, lanes) for side in (up, down, y)]

    def join(px, py, part, lanes):
        for k in range(4):
            qx, qy = (px, k) if py is EVERY else (k, py)
            pair[qx, qy, part, :, lanes] = add(
                g_ref[qx, qy, core, part, :, lanes], across[qx, qy, part, :, lanes]
            ).astype(BF16)

    def send_far(lanes):
        join(far_x, EVERY, 0, lanes)
        join(EVERY, far_y, 1, lanes)
        return [
            start(pair.at[far_x, LOW, 0, :, lanes], one.at[0, :, :, lanes], to_right),
            start(pair.at[far_x, HIGH, 0, :, lanes], one.at[1, :, :, lanes], to_left),
            start(pair.at[LOW, far_y, 1, :, lanes], one.at[2, :, :, lanes], to_up),
            start(pair.at[HIGH, far_y, 1, :, lanes], one.at[3, :, :, lanes], to_down),
        ]

    admit(everyone)
    far, rest = meet_all(early)


    def close(s):
        at = slice(s * SPAN, s * SPAN + SPAN)
        d_normed = dot(dpre_s[at, 0:512], w_ref[:, 512:1024], 1, 1)
        for part in range(1, 4):
            lanes = slice(part * 512, part * 512 + 512)
            wide = slice(part * 512 + 512, part * 512 + 1024)
            d_normed = d_normed + dot(dpre_s[at, lanes], w_ref[:, wide], 1, 1)
        normed, scale = moments(emb_s[at, :].astype(F32))
        back = norm_back(d_normed.astype(BF16).astype(F32), normed, scale)
        d_emb = (demb_s[at, :].astype(F32) + back).astype(BF16)
        demb_s[at, :] = d_emb
        d_rows = dot(d_emb, proj, 1, 1)
        table = cols_ref[at, 1:2]
        rank = cols_ref[at, 3:4]
        lane = lax.broadcasted_iota(I32, (SPAN, half), 1)
        kind = jnp.where(lane < 64, 0.0, 1.0)
        for k in range(2):
            match = rank == float(k)
            low = k * 128
            place_s[at, low : low + 128] = jnp.where(
                (table == kind) & match, d_rows[:, 0:128], 0.0
            ).astype(BF16)
            place_s[at, 256 + low : 384 + low] = jnp.where(
                (table == 2.0) & match, d_rows[:, 128:256], 0.0
            ).astype(BF16)
            low = 512 + k * 256
            place_s[at, low : low + 256] = jnp.where(
                (table == 3.0) & match, d_rows[:, 256:512], 0.0
            ).astype(BF16)

    close(0)
    finish(far)
    steps = send_far(early)
    close(1)
    g_ref[:, :, :, :, :, 0:512] = term(dot(rows_s[...], demb_s[...], 0, 0))
    far, more = meet_all(late)
    owner = cols_ref[:, 0:1].astype(I32)
    hot = (owner == lax.broadcasted_iota(I32, (TOKENS, DEVICES), 1)).astype(BF16)
    first_ref[...] = dot(hot, place_s[:, 0:512], 0, 0).astype(BF16)
    swap.ready_high()
    high = swap.begin_high()
    finish(far)
    steps += send_far(late)
    second_ref[...] = dot(hot, place_s[:, 512:1024], 0, 0).astype(BF16).reshape(32, NZ, 512)
    swap.ready_low()
    low = swap.begin_low()
    finish(rest + more)
    for side in (right, left):
        join(side, EVERY, 0, EVERY)
    for side in (up, down):
        join(EVERY, side, 1, EVERY)
    finish(steps)
    for k in range(2):
        pair[right, k, 0] = add(pair[right, k, 0], one[0, k]).astype(BF16)
        pair[left, 2 + k, 0] = add(pair[left, 2 + k, 0], one[1, k]).astype(BF16)
        pair[k, up, 1] = add(pair[k, up, 1], one[2, k]).astype(BF16)
        pair[2 + k, down, 1] = add(pair[2 + k, down, 1], one[3, k]).astype(BF16)
    steps = [
        start(pair.at[right, :, 0], two.at[0], to_right),
        start(pair.at[left, :, 0], two.at[1], to_left),
        start(pair.at[:, up, 1], two.at[2], to_up),
        start(pair.at[:, down, 1], two.at[3], to_down),
    ]
    finish(low)
    low = swap.turn_low()
    join(x, EVERY, 0, EVERY)
    join(EVERY, y, 1, EVERY)
    finish(steps)
    for k in range(4):
        line[0, k] = add(pair[x, k, 0], two[0, k], two[1, k]).astype(BF16)
        line[1, k] = add(pair[k, y, 1], two[2, k], two[3, k]).astype(BF16)
    steps = [
        start(line.at[0, far_y, :, AHEAD], three.at[0], to_up),
        start(line.at[0, far_y, :, BEHIND], three.at[1], to_down),
        start(line.at[1, far_x, :, AHEAD], three.at[2], to_right),
        start(line.at[1, far_x, :, BEHIND], three.at[3], to_left),
    ]
    finish(high)
    high = swap.turn_high()
    finish(steps)
    line[0, up, :, AHEAD] = add(line[0, up, :, AHEAD], three[0]).astype(BF16)
    line[0, down, :, BEHIND] = add(line[0, down, :, BEHIND], three[1]).astype(BF16)
    line[1, right, :, AHEAD] = add(line[1, right, :, AHEAD], three[2]).astype(BF16)
    line[1, left, :, BEHIND] = add(line[1, left, :, BEHIND], three[3]).astype(BF16)
    finish(
        [
            start(line.at[0, up], four.at[0], to_up),
            start(line.at[0, down], four.at[1], to_down),
            start(line.at[1, right], four.at[2], to_right),
            start(line.at[1, left], four.at[3], to_left),
        ]
    )
    for q in range(NZ):
        lanes = pl.ds(q * 384, 384)
        parts[q, 0] = add(line[0, y, :, lanes], four[0, :, lanes], four[1, :, lanes]).astype(BF16)
        parts[q, 1] = add(line[1, x, :, lanes], four[2, :, lanes], four[3, :, lanes]).astype(BF16)
    steps = [start(parts.at[t[1]], column.at[i], t) for i, t in enumerate(swap.along_z)]
    finish(low)
    swap.end_low()
    finish(steps)
    mine[...] = add(parts[z], *[column[k] for k in range(NZ - 1)]).astype(BF16)
    steps = [start(mine, whole.at[z], t) for t in swap.along_z]
    whole[pl.ds(z, 1)] = mine[...][None]
    finish(high + steps)
    for half in range(2):
        for q in range(NZ):
            total_ref[half * 8 : half * 8 + 8, q * 384 : q * 384 + 384] = whole[q, half]
    store.wait()


def core(got, cols, weights, cotangent):
    def vmem(width, kind=BF16):
        return pltpu.VMEM((TOKENS, width), kind)

    return pl.pallas_call(
        core_kernel,
        out_shape=(
            jax.ShapeDtypeStruct((TOKENS, WIDTH), BF16),
            jax.ShapeDtypeStruct((2, 32, 8, 512), BF16),
            jax.ShapeDtypeStruct((16, 3072), BF16),
        ),
        in_specs=[VM, VM, ANY, ANY],
        out_specs=(ANY, VM, VM),
        scratch_shapes=[
            vmem(512), vmem(512), vmem(512), vmem(2048, F32), vmem(2048), vmem(512, F32),
            vmem(512), vmem(512), vmem(2048), vmem(512), vmem(1024),
            pltpu.VMEM((512, 3072), BF16), vmem(512), vmem(512),
            pltpu.SemaphoreType.DMA((4,)), pltpu.SemaphoreType.DMA,
            pltpu.VMEM((DEVICES, 512), BF16),
            pltpu.VMEM((32, 8, 512), BF16),
            pltpu.VMEM((4, 4, 2, 2, 8, 3072), BF16),
            pltpu.VMEM((4, 4, 2, 8, 3072), BF16),
            pltpu.VMEM((4, 4, 2, 8, 3072), BF16),
            pltpu.VMEM((4, 2, 8, 3072), BF16),
            pltpu.VMEM((4, 4, 8, 3072), BF16),
            pltpu.VMEM((2, 4, 8, 3072), BF16),
            pltpu.VMEM((4, 8, 1536), BF16),
            pltpu.VMEM((4, 8, 3072), BF16),
            pltpu.VMEM((8, 2, 8, 384), BF16),
            pltpu.VMEM((7, 2, 8, 384), BF16),
            pltpu.VMEM((2, 8, 384), BF16),
            pltpu.VMEM((8, 2, 8, 384), BF16),
        ]
        + SWAP_SHAPES
        + sems(126),
        compiler_params=comm_params(3),
        name="core",
    )(got, cols, weights, cotangent)


def shards(
    item_ids, table_ids, lengths, assignment,
    table_a, table_b, table_c, table_d,
    proj_weight, in_weight, out_weight, cotangent,
):
    got, full, wanted, cols = front(
        item_ids,
        table_ids,
        lengths,
        assignment,
        (proj_weight, in_weight, out_weight),
        (table_a.T, table_b.T, table_c, table_d),
    )
    output, arrived, totals = core(
        got.reshape(2, DEVICES, 512),
        cols,
        full.reshape(512, 3072),
        cotangent.reshape(TOKENS, WIDTH),
    )
    grads = scatter(arrived.reshape(2, DEVICES, 512), wanted, totals)
    return (
        output.reshape(2, SPAN, WIDTH),
        grads[0].T,
        grads[1].T,
        *grads[2:],
    )


def solution(mesh):
    both = ("dp", "table")
    return jax.shard_map(
        shards,
        mesh=mesh,
        in_specs=(
            P(both, None), P(both, None), P(both), P(both),
            P(both, None), P(both, None), P(both, None), P(both, None),
            P("dp", None), P("dp", None), P("dp", None), P(both, None, None),
        ),
        out_specs=(
            P(both, None, None),
            P(both, None), P(both, None), P(both, None), P(both, None),
            P("dp", None), P("dp", None), P("dp", None),
        ),
        check_vma=False,
    )
```
